32 devices in a mesh: grp: 1, win: 32 (over z, y, x, core).
Axes of the slice: x: 2, y: 2, z: 4, core: 2. Of those that a mesh axis runs over, the one named last changes fastest.
Arguments:
- tokens: bfloat16 [2, 8, 64, 96, 384], P('grp', None, None, 'win'), may hold values from -6 to 6
- w_upper: bfloat16 [384, 640], replicated, may hold values from -0.3125 to 0.3125
- w_surface: bfloat16 [384, 256], replicated, may hold values from -0.3125 to 0.3125
- bias: float32 [69], replicated, may hold values from -1 to 1
Outputs:
- fields: bfloat16 [2, 17664, 384], P('grp', 'win')
The draws below stay inside these ranges and needn't reach their ends.
All inputs are finite; a program needn't handle non-finite values.
Results may differ from the reference program's by a relative error of at most 0.0048.
Values may be sent and summed in bfloat16 or wider, within the bound.
A program may use at most 128 MiB of HBM per device.

```python
import jax
import jax.numpy as jnp
from jax import lax

D = 384
VARS_UP = 5
LEVELS = 13
VARS_SF = 4
PATCH = 4
MEMB = 2
LAT_TOK = 64
LON_DEV = 3
LEV_TOK = 8
NLON = 96
OUT_CH = 69
N_WIN = 32


def steps_of(key, dims, split, least, largest):
    level, own = 1.0, jax.random.fold_in(key, 6)
    for dim, parts in split:
        steps = jnp.exp(jax.random.uniform(jax.random.fold_in(own, dim), (parts,), jnp.float32, least / len(split), largest / len(split)))
        level = level * jnp.repeat(steps, dims[dim] // parts).reshape([-1 if axis == dim else 1 for axis in range(len(dims))])
    return level


def normal_values(own_key, extent, scale, most, cuts=(), held_as=jnp.bfloat16):
    entries = scale * jax.random.normal(own_key, extent, jnp.float32)
    if cuts:
        entries = entries * steps_of(own_key, extent, cuts, -0.22, 0.18)
    return jnp.clip(entries, -most, most).astype(held_as)


def setup_inputs(seed: int = 0, part: int = 0) -> dict:
    streams_of = jax.random.split(jax.random.key(seed), 5)
    own_keys = jax.random.split(jax.random.fold_in(streams_of[4], part), 5)
    return {
        "tokens": normal_values(own_keys[0], (MEMB, LEV_TOK, LAT_TOK, NLON, D), 1.0, 6.0, ((3, 32),)),
        "w_upper": normal_values(streams_of[1], (D, VARS_UP * 8 * PATCH * PATCH), D ** -0.5, 0.3125),
        "w_surface": normal_values(streams_of[2], (D, VARS_SF * 4 * PATCH * PATCH), D ** -0.5, 0.3125),
        "bias": jnp.clip(jax.random.uniform(streams_of[3], (OUT_CH,), jnp.float32, -1.0, 1.0), -1.0, 1.0),
    }


def intersection_add(values, axis):
    first = lax.index_in_dim(values, 0, axis + 1, keepdims=False)
    second = lax.index_in_dim(values, 1, axis + 1, keepdims=False)
    pad_first = [(0, 0)] * first.ndim
    pad_second = [(0, 0)] * first.ndim
    pad_first[axis] = (0, 1)
    pad_second[axis] = (1, 0)
    return jnp.pad(first, pad_first) + jnp.pad(second, pad_second)


def project(tokens, w_upper, w_surface):
    members, tok_levels, lat_rows, lon_cols, width = tokens.shape
    upper_levels = tok_levels - 1
    rim_width = PATCH // 2
    upper = jnp.einsum("mzijd,dn->mzijn", tokens[:, :upper_levels], w_upper, preferred_element_type=jnp.float32)
    upper = upper.reshape(members, upper_levels, lat_rows, lon_cols, VARS_UP, 2, 2, PATCH, 2, PATCH)
    upper = jnp.transpose(upper, (0, 4, 1, 5, 2, 6, 7, 3, 8, 9))
    upper = intersection_add(upper, 4)
    upper = intersection_add(upper, 6)
    upper = upper.reshape(members, VARS_UP, 2 * upper_levels, (lat_rows + 1) * PATCH, (lon_cols + 1) * PATCH)
    upper = upper[:, :, :LEVELS, rim_width:rim_width + lat_rows * PATCH]
    upper = upper.reshape(members, VARS_UP * LEVELS, lat_rows * PATCH, (lon_cols + 1) * PATCH)
    surface = jnp.einsum("mijd,dn->mijn", tokens[:, upper_levels], w_surface, preferred_element_type=jnp.float32)
    surface = surface.reshape(members, lat_rows, lon_cols, VARS_SF, 2, PATCH, 2, PATCH)
    surface = jnp.transpose(surface, (0, 3, 1, 4, 5, 2, 6, 7))
    surface = intersection_add(surface, 2)
    surface = intersection_add(surface, 4)
    surface = surface.reshape(members, VARS_SF, (lat_rows + 1) * PATCH, (lon_cols + 1) * PATCH)
    surface = surface[:, :, rim_width:rim_width + lat_rows * PATCH]
    joined = jnp.concatenate([upper, surface], axis=1).astype(jnp.bfloat16)
    return joined.reshape(members, -1, (lon_cols + 1) * PATCH)


def reference(tokens, w_upper, w_surface, bias):
    members = tokens.shape[0]
    lat_rows = tokens.shape[2]
    rim_width = PATCH // 2

    def one_window(window):
        start = (window * LON_DEV).astype(jnp.int32)
        piece = lax.dynamic_slice_in_dim(tokens, start, LON_DEV, 3)
        return project(piece, w_upper, w_surface)

    frames = lax.map(one_window, jnp.arange(N_WIN, dtype=jnp.int32))
    frame_width = frames.shape[3]
    inner = frames[:, :, :, rim_width:frame_width - rim_width].astype(jnp.float32)
    columns = inner.shape[3]
    from_left = jnp.roll(frames[:, :, :, frame_width - rim_width:], 1, axis=0).astype(jnp.float32)
    from_right = jnp.roll(frames[:, :, :, :rim_width], -1, axis=0).astype(jnp.float32)
    edges = ((0, 0), (0, 0), (0, 0))
    summed = inner + jnp.pad(from_left, edges + ((0, columns - rim_width),))
    summed = summed + jnp.pad(from_right, edges + ((columns - rim_width, 0),))
    bias_rows = jnp.repeat(bias, lat_rows * PATCH)
    image = (summed + bias_rows[None, None, :, None]).astype(jnp.bfloat16)
    image = jnp.transpose(image, (1, 2, 0, 3))
    return image.reshape(members, image.shape[1], N_WIN * columns)
```

```python
import functools

import jax
import jax.numpy as jnp
from jax import lax
from jax.experimental import pallas as pl
from jax.experimental.pallas import tpu as pltpu
from jax.sharding import PartitionSpec as P

VARS_UP = 5
LEVELS = 13
VARS_SF = 4
PATCH = 4
GROUP = 8
CHANNELS = VARS_UP * LEVELS + VARS_SF


def spans_of(owners, own_rows):
    return [
        (o * own_rows // PATCH, -(-(o + 1) * own_rows // PATCH)) for o in range(owners)
    ]


def selector(second, column):
    row = lax.broadcasted_iota(jnp.int32, (128, 128), 0)
    n = lax.broadcasted_iota(jnp.int32, (128, 128), 1)
    step = (n // 16) % 4 - column
    source = (n // 64) * 64 + (((n // 4) % 4 + 2 + 4 * second) % 8) * 8 + n % 4 + 4 * step
    hit = (row == source) & (step >= 0) & (step <= 1)
    return jnp.where(hit, 1.0, 0.0).astype(jnp.bfloat16)


def partner(me, r, windows):
    if windows & (windows - 1):
        return lax.rem(me + r, windows)
    return me ^ r


def kernel(
    plan, tok_hbm, wu_hbm, ws_hbm, bias_ref, out_ref,
    tok_ref, wu_ref, ws_ref, wb_ref, proj_ref, frame_ref, wire_ref, got_ref, place_ref, image_ref,
    load_sem, send_sem, recv_sem,
):
    members, tok_levels, lon_cols, lat_rows, width = tok_ref.shape
    windows, pad_rows, _ = wire_ref.shape
    upper_levels = tok_levels - 1
    up_tiles = wu_ref.shape[1] // 128
    sf_tiles = ws_ref.shape[1] // 128
    me = lax.axis_index("win")

    loads = [
        pltpu.make_async_copy(wu_hbm, wu_ref, load_sem.at[0]),
        pltpu.make_async_copy(ws_hbm, ws_ref, load_sem.at[1]),
        pltpu.make_async_copy(tok_hbm, tok_ref, load_sem.at[2]),
    ]
    for load in loads:
        load.start()

    barrier = pltpu.get_barrier_semaphore()

    def greet(r, carry):
        pl.semaphore_signal(
            barrier, inc=1, device_id={"win": partner(me, r, windows)},
            device_id_type=pl.DeviceIdType.MESH,
        )
        return carry

    lax.fori_loop(1, windows, greet, 0)

    own_rows, low_plan, high_plan = plan
    sel = jnp.concatenate(
        [selector(y, j) for j in range(lon_cols) for y in range(2)], axis=1
    )

    def spread(w):
        wide = jnp.dot(w, sel, preferred_element_type=jnp.float32).astype(jnp.bfloat16)
        for j in range(lon_cols):
            wb_ref[j * width : (j + 1) * width, :] = wide[:, j * 256 : (j + 1) * 256]

    lane = lax.broadcasted_iota(jnp.int32, (lat_rows, 128), 1)
    line = lax.broadcasted_iota(jnp.int32, (lat_rows, 128), 0)
    lower = (lane // 4) % 4 < 2
    low_lanes = lane < 64
    keep = line != jnp.where(lower, 0, lat_rows - 1)

    def image(y):
        first, second = y[:, :128], y[:, 128:]
        moved = jnp.where(
            lower, pltpu.roll(second, 1, 0), pltpu.roll(second, lat_rows - 1, 0)
        )
        return first + jnp.where(keep, moved, 0.0)

    def put(channel, block):
        start = pl.multiple_of(channel * lat_rows, 8)
        frame_ref[pl.ds(start, lat_rows), :] = block

    def multiply(z0, z1):
        rows = (z1 - z0) * lat_rows
        for m in range(members):
            total = None
            for j in range(lon_cols):
                part = jnp.dot(
                    tok_ref[m, z0:z1, j].reshape(rows, width),
                    wb_ref[j * width : (j + 1) * width, :],
                    preferred_element_type=jnp.float32,
                )
                total = part if total is None else total + part
            proj_ref[m, :rows] = total

    def merge(even_channel, odd_channel, i):
        one, two = (
            image(proj_ref[m, i * lat_rows : (i + 1) * lat_rows, :]) for m in range(members)
        )
        put(even_channel, jnp.where(low_lanes, one, pltpu.roll(two, 64, 1)))
        if odd_channel is not None:
            put(odd_channel, jnp.where(low_lanes, pltpu.roll(one, 64, 1), two))

    def copy_to(other):
        return pltpu.make_async_remote_copy(
            src_ref=wire_ref.at[other],
            dst_ref=got_ref.at[me],
            send_sem=send_sem.at[other],
            recv_sem=recv_sem.at[me],
            device_id={"win": other},
            device_id_type=pl.DeviceIdType.MESH,
        )

    def block_of(other):
        start = other * own_rows // PATCH
        return frame_ref[pl.ds(start, pad_rows), :].astype(jnp.bfloat16)

    low = me < windows // 2

    def deliver(slot):
        begin, count, more, extra = (
            jnp.where(low, a, b) for a, b in zip(low_plan[slot], high_plan[slot])
        )
        total = count + extra

        def owner(i):
            i = lax.rem(i + me, jnp.maximum(total, 1))
            return jnp.where(i < count, begin + i, more + i - count)

        def pack(i, carry):
            other = owner(i)
            wire_ref[other] = block_of(other)
            return carry

        def send(i, carry):
            other = owner(i)

            @pl.when(other != me)
            def _():
                copy_to(other).start()

            return carry

        lax.fori_loop(0, total, pack, 0)
        if slot == 0:
            pl.semaphore_wait(barrier, windows - 1)
        lax.fori_loop(0, total, send, 0)

    tail = CHANNELS * lat_rows
    frame_ref[tail:, :] = jnp.zeros((frame_ref.shape[0] - tail, 128), jnp.float32)
    loads[0].wait()
    for slot in range(up_tiles):
        t = jnp.where(low, up_tiles - 1 - slot, slot)
        spread(wu_ref[:, pl.ds(pl.multiple_of(t * 128, 128), 128)])
        if slot == 0:
            loads[1].wait()
            loads[2].wait()
        multiply(0, upper_levels)
        for z in range(upper_levels):
            even = t * LEVELS + 2 * z
            merge(even, even + 1 if 2 * z + 1 < LEVELS else None, z)
        if slot == 1:
            for u in range(sf_tiles):
                spread(ws_ref[:, u * 128 : (u + 1) * 128])
                multiply(upper_levels, tok_levels)
                even = VARS_UP * LEVELS + 2 * u
                merge(even, even + 1, 0)
        deliver(slot)
    got_ref[me] = block_of(me)

    tiles = image_ref.shape[1]
    lons = tiles * 128
    groups = windows // GROUP
    pitch = lons // windows
    row = lax.broadcasted_iota(jnp.int32, (128, GROUP * 128), 0)
    col = lax.broadcasted_iota(jnp.int32, (128, GROUP * 128), 1)
    target = row // 64 * 512 + (row // 4) % 4 * 128 + (row // 16) % 4 * 4 + row % 4

    def fill(i, carry):
        hit = col == target + i * pitch
        place_ref[pl.ds(pl.multiple_of(i * 128, 128), 128), :] = jnp.where(
            hit, 1.0, 0.0
        ).astype(jnp.bfloat16)
        return carry

    lax.fori_loop(0, GROUP, fill, 0)

    def arrived(source):
        pltpu.make_async_remote_copy(
            src_ref=wire_ref.at[source],
            dst_ref=got_ref.at[source],
            send_sem=send_sem.at[source],
            recv_sem=recv_sem.at[source],
            device_id={"win": source},
            device_id_type=pl.DeviceIdType.MESH,
        ).wait_recv()

    def gather(k, carry):
        g = partner(me // GROUP, k, groups)

        def wait_one(i, inner):
            source = g * GROUP + i

            @pl.when(source != me)
            def _():
                arrived(source)

            return inner

        lax.fori_loop(0, GROUP, wait_one, 0)
        stacked = jnp.concatenate([got_ref[g * GROUP + i] for i in range(GROUP)], axis=1)
        moved = jnp.dot(stacked, place_ref[...], preferred_element_type=jnp.float32)
        start = g * (GROUP * pitch) + (lons - PATCH // 2)
        shift = lax.rem(start, 128)
        tile = lax.rem(start // 128, tiles)
        after = lax.rem(tile + 1, tiles)
        first_part = lane_of_pad >= shift
        for m in range(members):
            for q in range(PATCH):
                at = (m * PATCH + q) * 128
                value = pltpu.roll(moved[:, at : at + 128], shift, 1)
                rows = pl.ds(q, pad_rows, stride=PATCH)
                image_ref[m, tile, rows, :] += jnp.where(first_part, value, 0.0)
                image_ref[m, after, rows, :] += jnp.where(first_part, 0.0, value)
        return carry

    lane_of_pad = lax.broadcasted_iota(jnp.int32, (pad_rows, 128), 1)
    image_ref[...] = jnp.zeros(image_ref.shape, jnp.float32)
    lax.fori_loop(0, groups, gather, 0)

    first_row = me * own_rows
    height = lat_rows * PATCH
    row = first_row + lax.broadcasted_iota(jnp.int32, (own_rows, 128), 0)
    first = first_row // height
    last = CHANNELS - 1
    offsets = jnp.zeros((own_rows, 128), jnp.float32)
    for i in range((own_rows - 1) // height + 2):
        channel = jnp.minimum(first + i, last)
        begins = (first + i) * height
        offsets = jnp.where(row >= begins, bias_ref[channel], offsets)
    begin = 0 if own_rows % PATCH == 0 else lax.rem(first_row, PATCH)
    for m in range(members):
        for tile in range(tiles):
            rows = image_ref[m, tile, pl.ds(begin, own_rows), :]
            out_ref[m, :, tile * 128 : (tile + 1) * 128] = (rows + offsets).astype(jnp.bfloat16)

    def sent(r, carry):
        copy_to(partner(me, r, windows)).wait_send()
        return carry

    lax.fori_loop(1, windows, sent, 0)


def plan_of(spans, lat_rows, tiles):
    owners, depth = len(spans), LEVELS * lat_rows
    surface = tiles * depth
    inner = [o for o in range(owners) if spans[o][1] <= surface]
    low, high = [], []
    done_low, done_high = inner[-1] + 1, 0
    for slot in range(tiles):
        floor = (tiles - 1 - slot) * depth
        begin = min(o for o in range(owners) if spans[o][0] >= floor)
        begin = min(begin, done_low)
        extra = owners - inner[-1] - 1 if slot == 1 else 0
        low.append((begin, done_low - begin, inner[-1] + 1, extra))
        done_low = begin
        ready = sum(1 for lo, hi in spans if hi <= (slot + 1) * depth)
        ready = owners if slot == tiles - 1 else ready
        high.append((done_high, ready - done_high, 0, 0))
        done_high = ready
    return low, high


def body(tokens, w_upper, w_surface, bias):
    members, tok_levels, lat_rows, lon_cols, width = tokens.shape
    windows = lax.axis_size("win")
    own_rows = CHANNELS * lat_rows * PATCH // windows
    lons = windows * lon_cols * PATCH
    spans = spans_of(windows, own_rows)
    pad_rows = -(-max(hi - lo for lo, hi in spans) // 16) * 16
    frame_rows = -(-(spans[-1][0] + pad_rows) // 8) * 8
    low_plan, high_plan = plan_of(spans, lat_rows, w_upper.shape[1] // 128)
    bf16, f32 = jnp.bfloat16, jnp.float32
    by_lon = jnp.transpose(tokens, (0, 1, 3, 2, 4))
    return pl.pallas_call(
        functools.partial(kernel, (own_rows, low_plan, high_plan)),
        out_shape=pltpu.VMEM((members, own_rows, lons), bf16),
        in_specs=[pl.BlockSpec(memory_space=pltpu.HBM)] * 3
        + [pl.BlockSpec(memory_space=pltpu.SMEM)],
        out_specs=pl.BlockSpec(memory_space=pltpu.VMEM),
        scratch_shapes=[
            pltpu.VMEM(by_lon.shape, bf16),
            pltpu.VMEM(w_upper.shape, bf16),
            pltpu.VMEM(w_surface.shape, bf16),
            pltpu.VMEM((lon_cols * width, 256), bf16),
            pltpu.VMEM((members, (tok_levels - 1) * lat_rows, 256), f32),
            pltpu.VMEM((frame_rows, 128), f32),
            pltpu.VMEM((windows, pad_rows, 128), bf16),
            pltpu.VMEM((windows, pad_rows, 128), bf16),
            pltpu.VMEM((GROUP * 128, GROUP * 128), bf16),
            pltpu.VMEM((members, lons // 128, pad_rows * PATCH, 128), f32),
            pltpu.SemaphoreType.DMA((3,)),
            pltpu.SemaphoreType.DMA((windows,)),
            pltpu.SemaphoreType.DMA((windows,)),
        ],
        compiler_params=pltpu.CompilerParams(
            collective_id=0, has_side_effects=True, vmem_limit_bytes=65 * 1000 * 1000
        ),
    )(by_lon, w_upper, w_surface, bias)


def solution(mesh):
    placed = (P("grp", None, None, "win", None), P(), P(), P())
    return jax.shard_map(
        body, mesh=mesh, in_specs=placed, out_specs=P("grp", "win", None), check_vma=False
    )
```

```python
import functools

import jax
import jax.numpy as jnp
from jax import lax
from jax.experimental import pallas as pl
from jax.experimental.pallas import tpu as pltpu
from jax.sharding import PartitionSpec as P

VARS_UP = 5
LEVELS = 13
VARS_SF = 4
PATCH = 4
GROUP = 8
CHANNELS = VARS_UP * LEVELS + VARS_SF


def spans_of(owners, own_rows):
    return [
        (o * own_rows // PATCH, -(-(o + 1) * own_rows // PATCH)) for o in range(owners)
    ]


def place_of(lane):
    u = lane % 64
    own = u < 48
    q = jnp.where(own, jnp.where(u >= 24, 2, 0) + jnp.where(u % 24 >= 12, 1, 0), (u - 48) // 4)
    column = jnp.where(own, u - 12 * q, 12 + u % 4)
    return q, column, own


def selector(second, token):
    row = lax.broadcasted_iota(jnp.int32, (128, 128), 0)
    n = lax.broadcasted_iota(jnp.int32, (128, 128), 1)
    q, column, _ = place_of(n)
    k = column - PATCH * token
    source = n // 64 * 64 + (q + 2 + 4 * second) % 8 * 8 + k
    hit = (row == source) & (k >= 0) & (k < 2 * PATCH)
    return jnp.where(hit, 1.0, 0.0).astype(jnp.bfloat16)


def partner(me, r, windows):
    if windows & (windows - 1):
        return lax.rem(me + r, windows)
    return me ^ r


def kernel(
    plan, tok_hbm, wu_hbm, ws_hbm, bias_ref, out_ref,
    tok_ref, wu_ref, ws_ref, wb_ref, proj_ref, frame_ref, wire_ref, got_ref, edge_ref, side_ref, spot_ref,
    place_ref, image_ref, load_sem, send_sem, recv_sem, edge_sem,
):
    members, tok_levels, lon_cols, lat_rows, width = tok_ref.shape
    windows, pad_rows, _ = wire_ref.shape
    half = windows // 2
    upper_levels = tok_levels - 1
    up_tiles = wu_ref.shape[1] // 128
    sf_tiles = ws_ref.shape[1] // 128
    me = lax.axis_index("win")
    own_rows, main_rows, low_plan, high_plan = plan
    tail_rows = pad_rows - main_rows

    loads = [
        pltpu.make_async_copy(wu_hbm, wu_ref, load_sem.at[0]),
        pltpu.make_async_copy(ws_hbm, ws_ref, load_sem.at[1]),
        pltpu.make_async_copy(tok_hbm, tok_ref, load_sem.at[2]),
    ]
    for load in loads:
        load.start()

    barrier = pltpu.get_barrier_semaphore()

    def greet(r, carry):
        pl.semaphore_signal(
            barrier, inc=1, device_id={"win": partner(me, r, windows)},
            device_id_type=pl.DeviceIdType.MESH,
        )
        return carry

    lax.fori_loop(1, windows, greet, 0)

    sel = jnp.concatenate(
        [selector(y, j) for j in range(lon_cols) for y in range(2)], axis=1
    )

    def spread(w):
        wide = jnp.dot(w, sel, preferred_element_type=jnp.float32).astype(jnp.bfloat16)
        for j in range(lon_cols):
            wb_ref[j * width : (j + 1) * width, :] = wide[:, j * 256 : (j + 1) * 256]

    lane = lax.broadcasted_iota(jnp.int32, (lat_rows, 128), 1)
    line = lax.broadcasted_iota(jnp.int32, (lat_rows, 128), 0)
    lane_q, _, own_lane = place_of(lane)
    lower = lane_q < 2
    low_lanes = lane < 64
    keep = line != jnp.where(lower, 0, lat_rows - 1)

    def own_lanes(rows):
        return lax.broadcasted_iota(jnp.int32, (rows, 128), 1) % 64 < 48

    def chunk_lanes(rows, c):
        return lax.broadcasted_iota(jnp.int32, (rows, 128), 1) % 64 // 16 == c

    def image(y):
        first, second = y[:, :128], y[:, 128:]
        moved = jnp.where(
            lower, pltpu.roll(second, 1, 0), pltpu.roll(second, lat_rows - 1, 0)
        )
        return first + jnp.where(keep, moved, 0.0)

    def put(channel, block):
        start = pl.multiple_of(channel * lat_rows, 8)
        frame_ref[pl.ds(start, lat_rows), :] = block + jnp.where(own_lane, bias_ref[channel], 0.0)

    def multiply(z0, z1):
        rows = (z1 - z0) * lat_rows
        for m in range(members):
            total = None
            for j in range(lon_cols):
                part = jnp.dot(
                    tok_ref[m, z0:z1, j].reshape(rows, width),
                    wb_ref[j * width : (j + 1) * width, :],
                    preferred_element_type=jnp.float32,
                )
                total = part if total is None else total + part
            proj_ref[m, :rows] = total

    def merge(even_channel, odd_channel, i):
        one, two = (
            image(proj_ref[m, i * lat_rows : (i + 1) * lat_rows, :]) for m in range(members)
        )
        put(even_channel, jnp.where(low_lanes, one, pltpu.roll(two, 64, 1)))
        if odd_channel is not None:
            put(odd_channel, jnp.where(low_lanes, pltpu.roll(one, 64, 1), two))

    left_open = lax.rem(me, half) == 0
    right_open = lax.rem(me + 1, half) == 0

    def edge_copy(index, rows):
        return pltpu.make_async_remote_copy(
            src_ref=edge_ref.at[index, 0:rows],
            dst_ref=side_ref.at[index, 0:rows],
            send_sem=edge_sem.at[0, index],
            recv_sem=edge_sem.at[1, index],
            device_id={"win": lax.rem(me + 1, windows)},
            device_id_type=pl.DeviceIdType.MESH,
        )

    def give_edge(index, base, count):
        rows = count // 4
        packed = frame_ref[pl.ds(pl.multiple_of(base + 3 * rows, 8), rows), :]
        for c in range(3):
            part = frame_ref[pl.ds(pl.multiple_of(base + c * rows, 8), rows), :]
            packed = jnp.where(chunk_lanes(rows, c), pltpu.roll(part, 80 + 16 * c, 1), packed)
        edge_ref[index, 0:rows] = packed.astype(jnp.bfloat16)

    def send_edge(index, count):
        @pl.when(jnp.logical_not(right_open))
        def _():
            edge_copy(index, count // 4).start()

    def take_edge(index, base, count):
        rows = count // 4

        @pl.when(jnp.logical_not(left_open))
        def _():
            edge_copy(index, rows).wait_recv()
            moved = jnp.dot(
                side_ref[index, 0:rows], spot_ref[...], preferred_element_type=jnp.float32
            )
            for c in range(4):
                at = pl.ds(pl.multiple_of(base + c * rows, 8), rows)
                frame_ref[at, :] += moved[:, c * 128 : (c + 1) * 128]

    def rows_of(window):
        return lax.rem(window + 1, half) == 0

    def copy_of(source, other, rows):
        return pltpu.make_async_remote_copy(
            src_ref=wire_ref.at[other, 0:rows],
            dst_ref=got_ref.at[source, 0:rows],
            send_sem=send_sem.at[other],
            recv_sem=recv_sem.at[source],
            device_id={"win": other},
            device_id_type=pl.DeviceIdType.MESH,
        )

    def either(is_open, run):
        @pl.when(is_open)
        def _():
            run(pad_rows)

        @pl.when(jnp.logical_not(is_open))
        def _():
            run(main_rows)

    def pack_into(ref, index, other):
        start = other * own_rows // PATCH
        main = frame_ref[pl.ds(start, main_rows), :]
        tail = frame_ref[pl.ds(start + main_rows, tail_rows), :]
        parts = [pltpu.roll(tail, 48 - 16 * c, 1) for c in range(3)]
        if main_rows > 3 * tail_rows:
            parts.append(main[3 * tail_rows :])
        kept = own_lanes(main_rows) | right_open
        ref[index, 0:main_rows] = jnp.where(kept, main, jnp.concatenate(parts, axis=0)).astype(
            jnp.bfloat16
        )
        ref[index, main_rows:pad_rows] = tail.astype(jnp.bfloat16)

    low = me < half

    def deliver(slot):
        begin, count, more, extra = (
            jnp.where(low, a, b) for a, b in zip(low_plan[slot], high_plan[slot])
        )
        total = count + extra

        def owner(i):
            i = lax.rem(i + me, jnp.maximum(total, 1))
            return jnp.where(i < count, begin + i, more + i - count)

        def send(i, carry):
            other = owner(i)

            @pl.when(other != me)
            def _():
                pack_into(wire_ref, other, other)
                either(right_open, lambda rows: copy_of(me, other, rows).start())

            return carry

        lax.fori_loop(0, total, send, 0)

    def clear(i, carry):
        frame_ref[pl.ds(pl.multiple_of(i * 8, 8), 8), :] = jnp.zeros((8, 128), jnp.float32)
        return carry

    lax.fori_loop(0, frame_ref.shape[0] // 8, clear, 0)
    from_row = lax.broadcasted_iota(jnp.int32, spot_ref.shape, 0)
    to_col = lax.broadcasted_iota(jnp.int32, spot_ref.shape, 1)
    to_lane = from_row // 64 * 64 + from_row % 16 // 4 * 12 + from_row % 4
    spot_ref[...] = jnp.where(
        to_col == from_row % 64 // 16 * 128 + to_lane, 1.0, 0.0
    ).astype(jnp.bfloat16)

    depth = LEVELS * lat_rows
    surface = VARS_UP * depth
    shallow = VARS_SF * lat_rows

    def base_of(slot):
        t = jnp.where(low, up_tiles - 1 - slot, slot)
        return t, t * depth

    def settle(slot):
        take_edge(slot, base_of(slot)[1], depth)
        if slot == 1:
            take_edge(up_tiles, surface, shallow)
        deliver(slot)

    loads[0].wait()
    for slot in range(up_tiles):
        t, base = base_of(slot)
        spread(wu_ref[:, pl.ds(pl.multiple_of(t * 128, 128), 128)])
        if slot == 0:
            loads[1].wait()
            loads[2].wait()
        multiply(0, upper_levels)
        for z in range(upper_levels):
            even = t * LEVELS + 2 * z
            merge(even, even + 1 if 2 * z + 1 < LEVELS else None, z)
        give_edge(slot, base, depth)
        if slot == 0:
            pl.semaphore_wait(barrier, windows - 1)
        send_edge(slot, depth)
        if slot == 1:
            for u in range(sf_tiles):
                spread(ws_ref[:, u * 128 : (u + 1) * 128])
                multiply(upper_levels, tok_levels)
                even = VARS_UP * LEVELS + 2 * u
                merge(even, even + 1, 0)
            give_edge(up_tiles, surface, shallow)
            send_edge(up_tiles, shallow)
        if slot > 0:
            settle(slot - 1)
    settle(up_tiles - 1)
    pack_into(got_ref, me, me)

    tiles = image_ref.shape[1]
    lons = tiles * 128
    groups = windows // GROUP
    pitch = lons // windows
    row = lax.broadcasted_iota(jnp.int32, (128, GROUP * 128), 0)
    col = lax.broadcasted_iota(jnp.int32, (128, GROUP * 128), 1)
    row_q, row_column, row_own = place_of(row)
    target = row // 64 * 512 + row_q * 128 + row_column

    def fill(i, carry):
        hit = (col == target + i * pitch) & (row_own | (i == GROUP - 1))
        place_ref[pl.ds(pl.multiple_of(i * 128, 128), 128), :] = jnp.where(
            hit, 1.0, 0.0
        ).astype(jnp.bfloat16)
        return carry

    lax.fori_loop(0, GROUP, fill, 0)

    def unpack(source, may_be_open):
        main = got_ref[source, 0:main_rows]
        tail = jnp.zeros((tail_rows, 128), jnp.float32)
        for c in range(3):
            part = got_ref[source, c * tail_rows : (c + 1) * tail_rows].astype(jnp.float32)
            part = pltpu.roll(part, 80 + 16 * c, 1)
            tail = jnp.where(chunk_lanes(tail_rows, c), part, tail)
        if may_be_open:
            is_open = rows_of(source)
            raw = got_ref[source, main_rows:pad_rows].astype(jnp.float32)
            tail = jnp.where(is_open, raw, tail)
            wide = jnp.where(own_lanes(main_rows) | is_open, main.astype(jnp.float32), 0.0)
            main = wide.astype(jnp.bfloat16)
        return jnp.concatenate([main, tail.astype(jnp.bfloat16)], axis=0)

    def gather(k, carry):
        g = partner(me // GROUP, k, groups)

        def wait_one(i, inner):
            source = g * GROUP + i

            @pl.when(source != me)
            def _():
                either(rows_of(source), lambda rows: copy_of(source, source, rows).wait_recv())

            return inner

        lax.fori_loop(0, GROUP, wait_one, 0)
        stacked = jnp.concatenate(
            [unpack(g * GROUP + i, i == GROUP - 1) for i in range(GROUP)], axis=1
        )
        moved = jnp.dot(stacked, place_ref[...], preferred_element_type=jnp.float32)
        start = g * (GROUP * pitch) + (lons - PATCH // 2)
        shift = lax.rem(start, 128)
        tile = lax.rem(start // 128, tiles)
        after = lax.rem(tile + 1, tiles)
        first_part = lane_of_pad >= shift
        for m in range(members):
            for q in range(PATCH):
                at = (m * PATCH + q) * 128
                value = pltpu.roll(moved[:, at : at + 128], shift, 1)
                rows = pl.ds(q, pad_rows, stride=PATCH)
                image_ref[m, tile, rows, :] += jnp.where(first_part, value, 0.0)
                image_ref[m, after, rows, :] += jnp.where(first_part, 0.0, value)
        return carry

    lane_of_pad = lax.broadcasted_iota(jnp.int32, (pad_rows, 128), 1)
    image_ref[...] = jnp.zeros(image_ref.shape, jnp.float32)
    lax.fori_loop(0, groups, gather, 0)

    begin = 0 if own_rows % PATCH == 0 else lax.rem(me * own_rows, PATCH)
    for m in range(members):
        for tile in range(tiles):
            rows = image_ref[m, tile, pl.ds(begin, own_rows), :]
            out_ref[m, :, tile * 128 : (tile + 1) * 128] = rows.astype(jnp.bfloat16)

    def sent(r, carry):
        other = partner(me, r, windows)
        either(right_open, lambda rows: copy_of(me, other, rows).wait_send())
        return carry

    lax.fori_loop(1, windows, sent, 0)

    @pl.when(jnp.logical_not(right_open))
    def _():
        for index in range(up_tiles):
            edge_copy(index, depth // 4).wait_send()
        edge_copy(up_tiles, shallow // 4).wait_send()


def rows_for(longest):
    main = 16
    while True:
        tail = max(16, -(-(longest - main) // 16) * 16)
        if 3 * tail <= main:
            return main, tail
        main += 16


def plan_of(spans, lat_rows, tiles):
    owners, depth = len(spans), LEVELS * lat_rows
    surface = tiles * depth
    inner = [o for o in range(owners) if spans[o][1] <= surface]
    low, high = [], []
    done_low, done_high = inner[-1] + 1, 0
    for slot in range(tiles):
        floor = (tiles - 1 - slot) * depth
        begin = min(o for o in range(owners) if spans[o][0] >= floor)
        begin = min(begin, done_low)
        extra = owners - inner[-1] - 1 if slot == 1 else 0
        low.append((begin, done_low - begin, inner[-1] + 1, extra))
        done_low = begin
        ready = sum(1 for lo, hi in spans if hi <= (slot + 1) * depth)
        ready = owners if slot == tiles - 1 else ready
        high.append((done_high, ready - done_high, 0, 0))
        done_high = ready
    return low, high


def body(tokens, w_upper, w_surface, bias):
    members, tok_levels, lat_rows, lon_cols, width = tokens.shape
    windows = lax.axis_size("win")
    own_rows = CHANNELS * lat_rows * PATCH // windows
    lons = windows * lon_cols * PATCH
    spans = spans_of(windows, own_rows)
    main_rows, tail_rows = rows_for(max(hi - lo for lo, hi in spans))
    pad_rows = main_rows + tail_rows
    frame_rows = -(-(spans[-1][0] + pad_rows) // 8) * 8
    low_plan, high_plan = plan_of(spans, lat_rows, w_upper.shape[1] // 128)
    edges = w_upper.shape[1] // 128 + 1
    bf16, f32 = jnp.bfloat16, jnp.float32
    by_lon = jnp.transpose(tokens, (0, 1, 3, 2, 4))
    return pl.pallas_call(
        functools.partial(kernel, (own_rows, main_rows, low_plan, high_plan)),
        out_shape=pltpu.VMEM((members, own_rows, lons), bf16),
        in_specs=[pl.BlockSpec(memory_space=pltpu.HBM)] * 3
        + [pl.BlockSpec(memory_space=pltpu.SMEM)],
        out_specs=pl.BlockSpec(memory_space=pltpu.VMEM),
        scratch_shapes=[
            pltpu.VMEM(by_lon.shape, bf16),
            pltpu.VMEM(w_upper.shape, bf16),
            pltpu.VMEM(w_surface.shape, bf16),
            pltpu.VMEM((lon_cols * width, 256), bf16),
            pltpu.VMEM((members, (tok_levels - 1) * lat_rows, 256), f32),
            pltpu.VMEM((frame_rows, 128), f32),
            pltpu.VMEM((windows, pad_rows, 128), bf16),
            pltpu.VMEM((windows, pad_rows, 128), bf16),
            pltpu.VMEM((edges, LEVELS * lat_rows // 4, 128), bf16),
            pltpu.VMEM((edges, LEVELS * lat_rows // 4, 128), bf16),
            pltpu.VMEM((128, 4 * 128), bf16),
            pltpu.VMEM((GROUP * 128, GROUP * 128), bf16),
            pltpu.VMEM((members, lons // 128, pad_rows * PATCH, 128), f32),
            pltpu.SemaphoreType.DMA((3,)),
            pltpu.SemaphoreType.DMA((windows,)),
            pltpu.SemaphoreType.DMA((windows,)),
            pltpu.SemaphoreType.DMA((2, edges)),
        ],
        compiler_params=pltpu.CompilerParams(
            collective_id=0, has_side_effects=True, vmem_limit_bytes=65 * 1000 * 1000
        ),
    )(by_lon, w_upper, w_surface, bias)


def solution(mesh):
    placed = (P("grp", None, None, "win", None), P(), P(), P())
    return jax.shard_map(
        body, mesh=mesh, in_specs=placed, out_specs=P("grp", "win", None), check_vma=False
    )
```

```python
import functools

import jax
import jax.numpy as jnp
from jax import lax
from jax.experimental import pallas as pl
from jax.experimental.pallas import tpu as pltpu
from jax.sharding import PartitionSpec as P

VARS_UP = 5
LEVELS = 13
VARS_SF = 4
PATCH = 4
GROUP = 8
TO_SPARE = (36, 32, 4)
CHANNELS = VARS_UP * LEVELS + VARS_SF


def spans_of(owners, own_rows):
    return [
        (o * own_rows // PATCH, -(-(o + 1) * own_rows // PATCH)) for o in range(owners)
    ]


def place_of(lane):
    return lane // 8 % 4, lane // 32 % 2 * 8 + lane % 8


def partner(me, r, windows):
    if windows & (windows - 1):
        return lax.rem(me + r, windows)
    return me ^ r


def kernel(
    plan, tok_hbm, wu_hbm, ws_hbm, bias_ref, out_ref,
    tok_ref, wu_ref, ws_ref, wb_ref, proj_ref, frame_ref, wire_ref, got_ref, edge_ref, side_ref, spot_ref,
    sel_ref, pick_ref,    place_ref, image_ref, load_sem, send_sem, recv_sem, edge_sem,
):
    members, tok_levels, lon_cols, lat_rows, width = tok_ref.shape
    windows, pad_rows, _ = wire_ref.shape
    half = windows // 2
    upper_levels = tok_levels - 1
    up_tiles = wu_ref.shape[1] // 128
    sf_tiles = ws_ref.shape[1] // 128
    me = lax.axis_index("win")
    own_rows, main_rows, low_plan, high_plan = plan
    tail_rows = pad_rows - main_rows

    last = lon_cols - 1
    loads = [
        pltpu.make_async_copy(wu_hbm, wu_ref, load_sem.at[0]),
        pltpu.make_async_copy(ws_hbm, ws_ref, load_sem.at[1]),
        pltpu.make_async_copy(tok_hbm.at[:, :, last], tok_ref.at[:, :, last], load_sem.at[2]),
        pltpu.make_async_copy(
            tok_hbm.at[:, :, 0:last], tok_ref.at[:, :, 0:last], load_sem.at[3]
        ),
    ]
    for load in loads:
        load.start()

    barrier = pltpu.get_barrier_semaphore()

    def greet(r, carry):
        pl.semaphore_signal(
            barrier, inc=1, device_id={"win": partner(me, r, windows)},
            device_id_type=pl.DeviceIdType.MESH,
        )
        return carry

    lax.fori_loop(1, windows, greet, 0)

    def iota(shape, axis):
        return lax.broadcasted_iota(jnp.int32, shape, axis)

    def one_hot(hit):
        return jnp.where(hit, 1.0, 0.0).astype(jnp.bfloat16)

    def second_of(lat, half):
        return (lat + 2 + 4 * half) % 8

    def source_of(tile, level, lat, lon):
        return tile * 128 + level * 64 + lat * 8 + lon

    for side in range(2):
        for near in range(2):
            row = iota((256, 256), 0)
            n = iota((256, 256), 1)
            k = side * 8 + n % 8 - PATCH * (side + near)
            lat = second_of(n // 8 % 4, n // 128)
            hit = row == source_of(n // 64 % 2, n // 32 % 2, lat, k)
            at = (2 * side + near) * 256
            sel_ref[:, at : at + 256] = one_hot(hit & (k >= 0) & (k < 2 * PATCH))
    row = iota(pick_ref.shape, 0)
    n = iota(pick_ref.shape, 1)
    lat = second_of(n // 4 % 4, n // 128)
    pick_ref[...] = one_hot(row == source_of(n // 32 % 4, n // 16 % 2, lat, n % 4 + PATCH))
    row = iota(spot_ref.shape, 0)
    n = iota(spot_ref.shape, 1)
    to_lane = row // 64 * 64 + row // 4 % 4 * 8 + row % 4
    spot_ref[...] = one_hot(n == row // 16 % 4 * 128 + to_lane)

    def spread(w):
        wide = jnp.dot(w, sel_ref[0 : w.shape[1], :], preferred_element_type=jnp.float32)
        for side in range(2):
            for near in range(2):
                at = (2 * side + near) * 256
                wb_ref[side, near * width : (near + 1) * width, :] = wide[
                    :, at : at + 256
                ].astype(jnp.bfloat16)

    lane = iota((lat_rows, 128), 1)
    line = iota((lat_rows, 128), 0)
    frame_lower = lane % 32 < 16
    edge_lower = lane % 16 < 8
    own_lane = place_of(lane)[1] < 12

    def own_lanes(rows):
        return place_of(iota((rows, 128), 1))[1] < 12

    def chunk_lanes(rows, c):
        return place_of(iota((rows, 128), 1))[1] // 4 == c

    def image(y, lower):
        first, second = y[:, :128], y[:, 128:]
        moved = jnp.where(
            lower, pltpu.roll(second, 1, 0), pltpu.roll(second, lat_rows - 1, 0)
        )
        keep = line != jnp.where(lower, 0, lat_rows - 1)
        return first + jnp.where(keep, moved, 0.0)

    def exchange(parts, wanted):
        at = iota(parts[0].shape, 1)
        low_half, even = at < 64, at // 32 % 2 == 0
        halves = []
        for h in range(-(-wanted // 2)):
            for a, b in ((parts[0], parts[2]), (parts[1], parts[3])):
                if h == 0:
                    halves.append(jnp.where(low_half, a, pltpu.roll(b, 64, 1)))
                else:
                    halves.append(jnp.where(low_half, pltpu.roll(a, 64, 1), b))
        out = []
        for p in range(wanted):
            a, b = halves[p // 2 * 2], halves[p // 2 * 2 + 1]
            if p % 2 == 0:
                out.append(jnp.where(even, a, pltpu.roll(b, 32, 1)))
            else:
                out.append(jnp.where(even, pltpu.roll(a, 96, 1), b))
        return out

    def put(channel, block):
        start = pl.multiple_of(channel * lat_rows, 8)
        frame_ref[pl.ds(start, lat_rows), :] = block + jnp.where(own_lane, bias_ref[channel], 0.0)

    def multiply(z0, z1):
        rows = (z1 - z0) * lat_rows
        for m in range(members):
            token = [tok_ref[m, z0:z1, j].reshape(rows, width) for j in range(lon_cols)]
            for side in range(2):
                proj_ref[m, side, 0:rows] = jnp.dot(
                    jnp.concatenate(token[side : side + 2], axis=1), wb_ref[side],
                    preferred_element_type=jnp.float32,
                )

    def merge(z, channels):
        at = slice(z * lat_rows, (z + 1) * lat_rows)
        parts = [
            image(proj_ref[m, side, at, :], frame_lower)
            for m in range(members)
            for side in range(2)
        ]
        for channel, block in zip(channels, exchange(parts, len(channels))):
            if channel is not None:
                put(channel, block)

    low = me < half

    def first_tile(slot):
        return jnp.where(low, max(up_tiles - 2 * (slot + 1), 0), 2 * slot)

    def tiles_of(slot):
        return min(2, up_tiles - 2 * slot)

    left_open = lax.rem(me, half) == 0
    right_open = lax.rem(me + 1, half) == 0

    def edge_copy(index, rows):
        return pltpu.make_async_remote_copy(
            src_ref=edge_ref.at[index, 0:rows],
            dst_ref=side_ref.at[index, 0:rows],
            send_sem=edge_sem.at[0, index],
            recv_sem=edge_sem.at[1, index],
            device_id={"win": lax.rem(me + 1, windows)},
            device_id_type=pl.DeviceIdType.MESH,
        )

    part_rows = lat_rows // 2
    edge_rows = upper_levels * part_rows

    def edges(w, z0, z1, put_edge):
        rows = (z1 - z0) * lat_rows
        weights = jnp.dot(w, pick_ref[0 : w.shape[1], :], preferred_element_type=jnp.float32)
        weights = weights.astype(jnp.bfloat16)
        for m in range(members):
            proj_ref[m, 0, 0:rows] = jnp.dot(
                tok_ref[m, z0:z1, last].reshape(rows, width), weights,
                preferred_element_type=jnp.float32,
            )
        for z in range(z1 - z0):
            parts = []
            for m in range(members):
                x = image(proj_ref[m, 0, z * lat_rows : (z + 1) * lat_rows, :], edge_lower)
                parts += [x[:part_rows], x[part_rows:]]
            for i, block in enumerate(exchange(parts, w.shape[1] // 128)):
                put_edge(i, z, block.astype(jnp.bfloat16))

    def make_edges():
        loads[0].wait()
        loads[2].wait()
        for v in range(0, up_tiles, 4):

            def put_upper(i, z, block):
                edge_ref[v + i, z * part_rows : (z + 1) * part_rows] = block

            edges(wu_ref[:, v * 128 : min(v + 4, up_tiles) * 128], 0, upper_levels, put_upper)
        loads[1].wait()

        def put_surface(i, z, block):
            edge_ref[up_tiles, i * part_rows : (i + 1) * part_rows] = block

        edges(ws_ref[...], upper_levels, tok_levels, put_surface)

    def send_edges():
        @pl.when(jnp.logical_not(right_open))
        def _():
            for slot in range(slots):
                for i in range(tiles_of(slot)):
                    edge_copy(first_tile(slot) + i, edge_rows).start()
                if slot == 0:
                    edge_copy(up_tiles, sf_tiles * part_rows).start()

    def take_edge(index, rows):
        edge_copy(index, rows).wait_recv()
        return jnp.dot(
            side_ref[index, 0:rows], spot_ref[...], preferred_element_type=jnp.float32
        )

    def add_rows(channel, h, block):
        at = pl.multiple_of(channel * lat_rows + h * part_rows, 8)
        frame_ref[pl.ds(at, part_rows), :] += block

    def take_upper(t):
        moved = take_edge(t, edge_rows)
        for z in range(upper_levels):
            for h in range(2):
                for l in range(min(2, LEVELS - 2 * z)):
                    lanes = (2 * h + l) * 128
                    block = moved[z * part_rows : (z + 1) * part_rows, lanes : lanes + 128]
                    add_rows(t * LEVELS + 2 * z + l, h, block)

    def take_surface():
        moved = take_edge(up_tiles, sf_tiles * part_rows)
        for i in range(sf_tiles):
            for h in range(2):
                for l in range(2):
                    lanes = (2 * h + l) * 128
                    block = moved[i * part_rows : (i + 1) * part_rows, lanes : lanes + 128]
                    add_rows(VARS_UP * LEVELS + 2 * i + l, h, block)

    def rows_of(window):
        return lax.rem(window + 1, half) == 0

    def copy_of(source, other, rows):
        return pltpu.make_async_remote_copy(
            src_ref=wire_ref.at[other, 0:rows],
            dst_ref=got_ref.at[source, 0:rows],
            send_sem=send_sem.at[other],
            recv_sem=recv_sem.at[source],
            device_id={"win": other},
            device_id_type=pl.DeviceIdType.MESH,
        )

    def either(is_open, run):
        @pl.when(is_open)
        def _():
            run(pad_rows)

        @pl.when(jnp.logical_not(is_open))
        def _():
            run(main_rows)

    def pack_into(ref, index, other):
        start = other * own_rows // PATCH
        main = frame_ref[pl.ds(start, main_rows), :]
        tail = frame_ref[pl.ds(start + main_rows, tail_rows), :]
        parts = [pltpu.roll(tail, shift, 1) for shift in TO_SPARE]
        if main_rows > 3 * tail_rows:
            parts.append(main[3 * tail_rows :])
        kept = own_lanes(main_rows) | right_open
        ref[index, 0:main_rows] = jnp.where(kept, main, jnp.concatenate(parts, axis=0)).astype(
            jnp.bfloat16
        )
        ref[index, main_rows:pad_rows] = tail.astype(jnp.bfloat16)

    def deliver(slot):
        begin, count, more, extra = (
            jnp.where(low, a, b) for a, b in zip(low_plan[slot], high_plan[slot])
        )
        total = count + extra

        def owner(i):
            i = lax.rem(i + me, jnp.maximum(total, 1))
            return jnp.where(i < count, begin + i, more + i - count)

        def send(i, carry):
            one, two = owner(2 * i), owner(jnp.minimum(2 * i + 1, total - 1))
            pack_into(wire_ref, one, one)
            pack_into(wire_ref, two, two)

            @pl.when(one != me)
            def _():
                either(right_open, lambda rows: copy_of(me, one, rows).start())

            @pl.when((two != me) & (2 * i + 1 < total))
            def _():
                either(right_open, lambda rows: copy_of(me, two, rows).start())

            return carry

        lax.fori_loop(0, (total + 1) // 2, send, 0)

    slots = -(-up_tiles // 2)
    tiles = image_ref.shape[1]
    lons = tiles * 128
    groups = windows // GROUP
    pitch = lons // windows
    row = iota((128, GROUP * 128), 0)
    col = iota((128, GROUP * 128), 1)
    row_q, row_column = place_of(row)
    target = row // 64 * 512 + row_q * 128 + row_column

    def fill(i, carry):
        hit = (col == target + i * pitch) & ((row_column < 12) | (i == GROUP - 1))
        place_ref[pl.ds(pl.multiple_of(i * 128, 128), 128), :] = one_hot(hit)
        return carry

    lax.fori_loop(0, GROUP, fill, 0)
    image_ref[...] = jnp.zeros(image_ref.shape, jnp.float32)
    frame_ref[...] = jnp.zeros(frame_ref.shape, jnp.float32)
    make_edges()
    pl.semaphore_wait(barrier, windows - 1)
    send_edges()
    for slot in range(slots):
        t, count = first_tile(slot), tiles_of(slot)
        spread(wu_ref[:, pl.ds(pl.multiple_of(t * 128, 128), count * 128)])
        if slot == 0:
            loads[3].wait()
        multiply(0, upper_levels)
        for z in range(upper_levels):
            merge(
                z,
                [
                    (t + i) * LEVELS + 2 * z + l if 2 * z + l < LEVELS else None
                    for i in range(count)
                    for l in range(2)
                ],
            )
        if slot == 1:
            spread(ws_ref[...])
            multiply(upper_levels, tok_levels)
            merge(0, [VARS_UP * LEVELS + v for v in range(VARS_SF)])

        @pl.when(jnp.logical_not(left_open))
        def _():
            for i in range(count):
                take_upper(t + i)
            if slot == 1:
                take_surface()

        deliver(slot)
    pack_into(got_ref, me, me)

    def unpack(source, may_be_open):
        main = got_ref[source, 0:main_rows]
        tail = jnp.zeros((tail_rows, 128), jnp.float32)
        for c in range(3):
            part = got_ref[source, c * tail_rows : (c + 1) * tail_rows].astype(jnp.float32)
            part = pltpu.roll(part, 128 - TO_SPARE[c], 1)
            tail = jnp.where(chunk_lanes(tail_rows, c), part, tail)
        if may_be_open:
            is_open = rows_of(source)
            raw = got_ref[source, main_rows:pad_rows].astype(jnp.float32)
            tail = jnp.where(is_open, raw, tail)
            wide = jnp.where(own_lanes(main_rows) | is_open, main.astype(jnp.float32), 0.0)
            main = wide.astype(jnp.bfloat16)
        return jnp.concatenate([main, tail.astype(jnp.bfloat16)], axis=0)

    def gather(k, carry):
        g = partner(me // GROUP, k, groups)

        def wait_one(i, inner):
            source = g * GROUP + i

            @pl.when(source != me)
            def _():
                either(rows_of(source), lambda rows: copy_of(source, source, rows).wait_recv())

            return inner

        lax.fori_loop(0, GROUP, wait_one, 0)
        stacked = jnp.concatenate(
            [unpack(g * GROUP + i, i == GROUP - 1) for i in range(GROUP)], axis=1
        )
        moved = jnp.dot(stacked, place_ref[...], preferred_element_type=jnp.float32)
        start = g * (GROUP * pitch) + (lons - PATCH // 2)
        shift = lax.rem(start, 128)
        tile = lax.rem(start // 128, tiles)
        after = lax.rem(tile + 1, tiles)
        first_part = lane_of_pad >= shift
        for m in range(members):
            for q in range(PATCH):
                at = (m * PATCH + q) * 128
                value = pltpu.roll(moved[:, at : at + 128], shift, 1)
                rows = pl.ds(q, pad_rows, stride=PATCH)
                image_ref[m, tile, rows, :] += jnp.where(first_part, value, 0.0)
                image_ref[m, after, rows, :] += jnp.where(first_part, 0.0, value)
        return carry

    lane_of_pad = lax.broadcasted_iota(jnp.int32, (pad_rows, 128), 1)
    lax.fori_loop(0, groups, gather, 0)

    begin = 0 if own_rows % PATCH == 0 else lax.rem(me * own_rows, PATCH)
    for m in range(members):
        for tile in range(tiles):
            rows = image_ref[m, tile, pl.ds(begin, own_rows), :]
            out_ref[m, :, tile * 128 : (tile + 1) * 128] = rows.astype(jnp.bfloat16)

    def sent(r, carry):
        other = partner(me, r, windows)
        either(right_open, lambda rows: copy_of(me, other, rows).wait_send())
        return carry

    lax.fori_loop(1, windows, sent, 0)

    @pl.when(jnp.logical_not(right_open))
    def _():
        for index in range(up_tiles):
            edge_copy(index, edge_rows).wait_send()
        edge_copy(up_tiles, sf_tiles * part_rows).wait_send()


def rows_for(longest):
    main = 16
    while True:
        tail = max(16, -(-(longest - main) // 16) * 16)
        if 3 * tail <= main:
            return main, tail
        main += 16


def plan_of(spans, lat_rows, tiles):
    owners, depth = len(spans), LEVELS * lat_rows
    surface, slots = tiles * depth, -(-tiles // 2)
    inner = [o for o in range(owners) if spans[o][1] <= surface]
    low, high = [], []
    done_low, done_high = inner[-1] + 1, 0
    for slot in range(slots):
        floor = max(tiles - 2 * (slot + 1), 0) * depth
        begin = min(o for o in range(owners) if spans[o][0] >= floor)
        begin = min(begin, done_low)
        extra = owners - inner[-1] - 1 if slot == 1 else 0
        low.append((begin, done_low - begin, inner[-1] + 1, extra))
        done_low = begin
        ready = sum(1 for lo, hi in spans if hi <= min(2 * (slot + 1), tiles) * depth)
        ready = owners if slot == slots - 1 else ready
        high.append((done_high, ready - done_high, 0, 0))
        done_high = ready
    return low, high


def body(tokens, w_upper, w_surface, bias):
    members, tok_levels, lat_rows, lon_cols, width = tokens.shape
    windows = lax.axis_size("win")
    own_rows = CHANNELS * lat_rows * PATCH // windows
    lons = windows * lon_cols * PATCH
    spans = spans_of(windows, own_rows)
    main_rows, tail_rows = rows_for(max(hi - lo for lo, hi in spans))
    pad_rows = main_rows + tail_rows
    frame_rows = -(-(spans[-1][0] + pad_rows) // 8) * 8
    low_plan, high_plan = plan_of(spans, lat_rows, w_upper.shape[1] // 128)
    edges = w_upper.shape[1] // 128 + 1
    bf16, f32 = jnp.bfloat16, jnp.float32
    by_lon = jnp.transpose(tokens, (0, 1, 3, 2, 4))
    return pl.pallas_call(
        functools.partial(kernel, (own_rows, main_rows, low_plan, high_plan)),
        out_shape=pltpu.VMEM((members, own_rows, lons), bf16),
        in_specs=[pl.BlockSpec(memory_space=pltpu.HBM)] * 3
        + [pl.BlockSpec(memory_space=pltpu.SMEM)],
        out_specs=pl.BlockSpec(memory_space=pltpu.VMEM),
        scratch_shapes=[
            pltpu.VMEM(by_lon.shape, bf16),
            pltpu.VMEM(w_upper.shape, bf16),
            pltpu.VMEM(w_surface.shape, bf16),
            pltpu.VMEM((2, 2 * width, 256), bf16),
            pltpu.VMEM((members, 2, (tok_levels - 1) * lat_rows, 256), f32),
            pltpu.VMEM((frame_rows, 128), f32),
            pltpu.VMEM((windows, pad_rows, 128), bf16),
            pltpu.VMEM((windows, pad_rows, 128), bf16),
            pltpu.VMEM((edges, (tok_levels - 1) * lat_rows // 2, 128), bf16),
            pltpu.VMEM((edges, (tok_levels - 1) * lat_rows // 2, 128), bf16),
            pltpu.VMEM((128, 4 * 128), bf16),
            pltpu.VMEM((256, 1024), bf16),
            pltpu.VMEM((512, 256), bf16),
            pltpu.VMEM((GROUP * 128, GROUP * 128), bf16),
            pltpu.VMEM((members, lons // 128, pad_rows * PATCH, 128), f32),
            pltpu.SemaphoreType.DMA((4,)),
            pltpu.SemaphoreType.DMA((windows,)),
            pltpu.SemaphoreType.DMA((windows,)),
            pltpu.SemaphoreType.DMA((2, edges)),
        ],
        compiler_params=pltpu.CompilerParams(
            collective_id=0, has_side_effects=True, vmem_limit_bytes=65 * 1000 * 1000
        ),
    )(by_lon, w_upper, w_surface, bias)


def solution(mesh):
    placed = (P("grp", None, None, "win", None), P(), P(), P())
    return jax.shard_map(
        body, mesh=mesh, in_specs=placed, out_specs=P("grp", "win", None), check_vma=False
    )
```

```python
import functools

import jax
import jax.numpy as jnp
from jax import lax
from jax.experimental import pallas as pl
from jax.experimental.pallas import tpu as pltpu
from jax.sharding import PartitionSpec as P

VARS_UP = 5
LEVELS = 13
VARS_SF = 4
PATCH = 4
GROUP = 8
TO_SPARE = (36, 32, 4)
CHANNELS = VARS_UP * LEVELS + VARS_SF


def spans_of(owners, own_rows):
    return [
        (o * own_rows // PATCH, -(-(o + 1) * own_rows // PATCH)) for o in range(owners)
    ]


def place_of(lane):
    return lane // 8 % 4, lane // 32 % 2 * 8 + lane % 8


def partner(me, r, windows):
    if windows & (windows - 1):
        return lax.rem(me + r, windows)
    return me ^ r


def kernel(
    plan, tok_hbm, wu_hbm, ws_hbm, bias_ref, out_ref,
    tok_ref, wu_ref, ws_ref, wb_ref, proj_ref, frame_ref, wire_ref, got_ref, edge_ref, side_ref, spot_ref,
    sel_ref, pick_ref,    place_ref, image_ref, wide_ref, load_sem, send_sem, recv_sem, edge_sem,
):
    members, tok_levels, lon_cols, lat_rows, width = tok_ref.shape
    windows, pad_rows, _ = wire_ref.shape
    half = windows // 2
    upper_levels = tok_levels - 1
    up_tiles = wu_ref.shape[1] // 128
    sf_tiles = ws_ref.shape[1] // 128
    me = lax.axis_index("win")
    own_rows, main_rows, extra_rows, sends = plan

    last = lon_cols - 1
    loads = [
        pltpu.make_async_copy(wu_hbm, wu_ref, load_sem.at[0]),
        pltpu.make_async_copy(ws_hbm, ws_ref, load_sem.at[1]),
        pltpu.make_async_copy(tok_hbm.at[:, :, last], tok_ref.at[:, :, last], load_sem.at[2]),
        pltpu.make_async_copy(
            tok_hbm.at[:, :, 0:last], tok_ref.at[:, :, 0:last], load_sem.at[3]
        ),
    ]
    for load in loads:
        load.start()

    barrier = pltpu.get_barrier_semaphore()

    def greet(r, carry):
        pl.semaphore_signal(
            barrier, inc=1, device_id={"win": partner(me, r, windows)},
            device_id_type=pl.DeviceIdType.MESH,
        )
        return carry

    lax.fori_loop(1, windows, greet, 0)

    def iota(shape, axis):
        return lax.broadcasted_iota(jnp.int32, shape, axis)

    def one_hot(hit):
        return jnp.where(hit, 1.0, 0.0).astype(jnp.bfloat16)

    def second_of(lat, half):
        return (lat + 2 + 4 * half) % 8

    def source_of(tile, level, lat, lon):
        return tile * 128 + level * 64 + lat * 8 + lon

    for side in range(2):
        for near in range(2):
            row = iota((256, 256), 0)
            n = iota((256, 256), 1)
            k = side * 8 + n % 8 - PATCH * (side + near)
            lat = second_of(n // 8 % 4, n // 128)
            hit = row == source_of(n // 64 % 2, n // 32 % 2, lat, k)
            at = (2 * side + near) * 256
            sel_ref[:, at : at + 256] = one_hot(hit & (k >= 0) & (k < 2 * PATCH))
    row = iota(pick_ref.shape, 0)
    n = iota(pick_ref.shape, 1)
    lat = second_of(n // 4 % 4, n // 128)
    pick_ref[...] = one_hot(row == source_of(n // 32 % 4, n // 16 % 2, lat, n % 4 + PATCH))
    row = iota(spot_ref.shape, 0)
    n = iota(spot_ref.shape, 1)
    to_lane = row // 64 * 64 + row // 4 % 4 * 8 + row % 4
    spot_ref[...] = one_hot(n == row // 16 % 4 * 128 + to_lane)

    def spread(w):
        wide = jnp.dot(w, sel_ref[0 : w.shape[1], :], preferred_element_type=jnp.float32)
        for side in range(2):
            for near in range(2):
                at = (2 * side + near) * 256
                wb_ref[side, near * width : (near + 1) * width, :] = wide[
                    :, at : at + 256
                ].astype(jnp.bfloat16)

    lane = iota((lat_rows, 128), 1)
    line = iota((lat_rows, 128), 0)
    frame_lower = lane % 32 < 16
    edge_lower = lane % 16 < 8
    own_lane = place_of(lane)[1] < 12

    def own_lanes(rows):
        return place_of(iota((rows, 128), 1))[1] < 12

    def chunk_lanes(rows, c):
        return place_of(iota((rows, 128), 1))[1] // 4 == c

    def image(y, lower):
        first, second = y[:, :128], y[:, 128:]
        moved = jnp.where(
            lower, pltpu.roll(second, 1, 0), pltpu.roll(second, lat_rows - 1, 0)
        )
        keep = line != jnp.where(lower, 0, lat_rows - 1)
        return first + jnp.where(keep, moved, 0.0)

    def exchange(parts, wanted):
        at = iota(parts[0].shape, 1)
        low_half, even = at < 64, at // 32 % 2 == 0
        halves = []
        for h in range(-(-wanted // 2)):
            for a, b in ((parts[0], parts[2]), (parts[1], parts[3])):
                if h == 0:
                    halves.append(jnp.where(low_half, a, pltpu.roll(b, 64, 1)))
                else:
                    halves.append(jnp.where(low_half, pltpu.roll(a, 64, 1), b))
        out = []
        for p in range(wanted):
            a, b = halves[p // 2 * 2], halves[p // 2 * 2 + 1]
            if p % 2 == 0:
                out.append(jnp.where(even, a, pltpu.roll(b, 32, 1)))
            else:
                out.append(jnp.where(even, pltpu.roll(a, 96, 1), b))
        return out

    def put(channel, block):
        start = pl.multiple_of(channel * lat_rows, 8)
        frame_ref[pl.ds(start, lat_rows), :] = block + jnp.where(own_lane, bias_ref[channel], 0.0)

    def multiply(z0, z1):
        rows = (z1 - z0) * lat_rows
        for m in range(members):
            token = [tok_ref[m, z0:z1, j].reshape(rows, width) for j in range(lon_cols)]
            for side in range(2):
                proj_ref[m, side, 0:rows] = jnp.dot(
                    jnp.concatenate(token[side : side + 2], axis=1), wb_ref[side],
                    preferred_element_type=jnp.float32,
                )

    def merge(z, channels):
        at = slice(z * lat_rows, (z + 1) * lat_rows)
        parts = [
            image(proj_ref[m, side, at, :], frame_lower)
            for m in range(members)
            for side in range(2)
        ]
        for channel, block in zip(channels, exchange(parts, len(channels))):
            if channel is not None:
                put(channel, block)

    low = me < half

    def first_tile(slot):
        low_tiles, high_tiles = tile_order(up_tiles)
        return jnp.where(low, low_tiles[slot], high_tiles[slot])

    def tiles_of(slot):
        return min(2, up_tiles - 2 * slot)

    left_open = lax.rem(me, half) == 0
    right_open = lax.rem(me + 1, half) == 0

    def edge_copy(index, rows):
        return pltpu.make_async_remote_copy(
            src_ref=edge_ref.at[index, 0:rows],
            dst_ref=side_ref.at[index, 0:rows],
            send_sem=edge_sem.at[0, index],
            recv_sem=edge_sem.at[1, index],
            device_id={"win": lax.rem(me + 1, windows)},
            device_id_type=pl.DeviceIdType.MESH,
        )

    part_rows = lat_rows // 2
    edge_rows = upper_levels * part_rows

    def edges(w, z0, z1, put_edge):
        rows = (z1 - z0) * lat_rows
        weights = jnp.dot(w, pick_ref[0 : w.shape[1], :], preferred_element_type=jnp.float32)
        weights = weights.astype(jnp.bfloat16)
        for m in range(members):
            proj_ref[m, 0, 0:rows] = jnp.dot(
                tok_ref[m, z0:z1, last].reshape(rows, width), weights,
                preferred_element_type=jnp.float32,
            )
        for z in range(z1 - z0):
            parts = []
            for m in range(members):
                x = image(proj_ref[m, 0, z * lat_rows : (z + 1) * lat_rows, :], edge_lower)
                parts += [x[:part_rows], x[part_rows:]]
            for i, block in enumerate(exchange(parts, w.shape[1] // 128)):
                put_edge(i, z, block.astype(jnp.bfloat16))

    def make_edges():
        for load in loads[:3]:
            load.wait()
        for v in range(0, up_tiles, 4):

            def put_upper(i, z, block):
                edge_ref[v + i, z * part_rows : (z + 1) * part_rows] = block

            edges(wu_ref[:, v * 128 : min(v + 4, up_tiles) * 128], 0, upper_levels, put_upper)

        def put_surface(i, z, block):
            edge_ref[up_tiles, i * part_rows : (i + 1) * part_rows] = block

        edges(ws_ref[...], upper_levels, tok_levels, put_surface)

    def send_edges():
        @pl.when(jnp.logical_not(right_open))
        def _():
            for slot in range(slots):
                for i in range(tiles_of(slot)):
                    edge_copy(first_tile(slot) + i, edge_rows).start()
                if slot == slots - 1:
                    edge_copy(up_tiles, sf_tiles * part_rows).start()

    def take_edge(index, rows):
        edge_copy(index, rows).wait_recv()
        return jnp.dot(
            side_ref[index, 0:rows], spot_ref[...], preferred_element_type=jnp.float32
        )

    def add_rows(channel, h, block):
        at = pl.multiple_of(channel * lat_rows + h * part_rows, 8)
        frame_ref[pl.ds(at, part_rows), :] += block

    def take_upper(t):
        moved = take_edge(t, edge_rows)
        for z in range(upper_levels):
            for h in range(2):
                for l in range(min(2, LEVELS - 2 * z)):
                    lanes = (2 * h + l) * 128
                    block = moved[z * part_rows : (z + 1) * part_rows, lanes : lanes + 128]
                    add_rows(t * LEVELS + 2 * z + l, h, block)

    def take_surface():
        moved = take_edge(up_tiles, sf_tiles * part_rows)
        for i in range(sf_tiles):
            for h in range(2):
                for l in range(2):
                    lanes = (2 * h + l) * 128
                    block = moved[i * part_rows : (i + 1) * part_rows, lanes : lanes + 128]
                    add_rows(VARS_UP * LEVELS + 2 * i + l, h, block)

    def rows_of(window):
        return lax.rem(window + 1, half) == 0

    def copy_of(source, other, rows):
        return pltpu.make_async_remote_copy(
            src_ref=wire_ref.at[other, 0:rows],
            dst_ref=got_ref.at[source, 0:rows],
            send_sem=send_sem.at[other],
            recv_sem=recv_sem.at[source],
            device_id={"win": other},
            device_id_type=pl.DeviceIdType.MESH,
        )

    def either(is_open, run):
        @pl.when(is_open)
        def _():
            run(pad_rows)

        @pl.when(jnp.logical_not(is_open))
        def _():
            run(main_rows)

    def pack_into(ref, index, other):
        start = other * own_rows // PATCH
        main = frame_ref[pl.ds(start, main_rows), :]
        tail = frame_ref[pl.ds(start + main_rows, pad_rows - main_rows), :]
        chunks = []
        for c in range(3):
            first = c * extra_rows // 8 * 8
            end = min(-(-(c + 1) * extra_rows // 8) * 8, main_rows) if c < 2 else main_rows
            rows = frame_ref[pl.ds(start + main_rows - c * extra_rows + first, end - first), :]
            chunks.append((first, pltpu.roll(rows, TO_SPARE[c], 1)))
        line_of_8 = iota((8, 128), 0)
        spare = []
        for at in range(0, main_rows, 8):
            block = None
            for c, (first, rows) in enumerate(chunks):
                if first <= at < first + rows.shape[0]:
                    part = rows[at - first : at - first + 8]
                    begins = line_of_8 >= c * extra_rows - at
                    block = part if block is None else jnp.where(begins, part, block)
            spare.append(block)
        kept = own_lanes(main_rows) | right_open
        main = jnp.where(kept, main, jnp.concatenate(spare, axis=0))
        ref[index] = jnp.concatenate([main, tail], axis=0).astype(jnp.bfloat16)

    pair_of_me = me // 2

    def serve(low_range, high_range):
        begin, end = (jnp.where(low, a, b) for a, b in zip(low_range, high_range))
        first_pair = begin // 2
        pairs = (end + 1) // 2 - first_pair

        def send(i, carry):
            pair = first_pair + lax.rem(i + pair_of_me, jnp.maximum(pairs, 1))
            one, two = 2 * pair, 2 * pair + 1
            first, second = jnp.maximum(one, begin), jnp.minimum(two, end - 1)
            pack_into(wire_ref, first, first)
            pack_into(wire_ref, second, second)

            @pl.when((one != me) & (one >= begin))
            def _():
                either(right_open, lambda rows: copy_of(me, one, rows).start())

            @pl.when((two != me) & (two < end))
            def _():
                either(right_open, lambda rows: copy_of(me, two, rows).start())

            return carry

        lax.fori_loop(0, pairs, send, 0)

    slots = -(-up_tiles // 2)
    tiles = image_ref.shape[1]
    lons = tiles * 128
    groups = windows // GROUP
    pitch = lons // windows
    row = iota((128, place_ref.shape[1]), 0)
    col = iota(row.shape, 1)
    row_q, row_column = place_of(row)
    target = row // 64 * 512 + row_q * 128 + row_column

    def fill(i, carry):
        hit = (col == target + i * pitch) & ((row_column < 12) | (i == GROUP - 1))
        place_ref[pl.ds(pl.multiple_of(i * 128, 128), 128), :] = one_hot(hit)
        return carry

    lax.fori_loop(0, GROUP, fill, 0)
    image_ref[...] = jnp.zeros(image_ref.shape, jnp.float32)
    frame_ref[...] = jnp.zeros(frame_ref.shape, jnp.float32)
    def spread_upper(slot):
        t, count = first_tile(slot), tiles_of(slot)
        spread(wu_ref[:, pl.ds(pl.multiple_of(t * 128, 128), count * 128)])

    def meet():
        pl.semaphore_wait(barrier, windows - 1)
        send_edges()

    make_edges()
    spread_upper(0)
    early = me < windows // 4
    pl.when(jnp.logical_not(early))(meet)
    loads[3].wait()
    for slot in range(slots):
        t, count = first_tile(slot), tiles_of(slot)
        if slot > 0:
            spread_upper(slot)
        multiply(0, upper_levels)
        for z in range(upper_levels):
            merge(
                z,
                [
                    (t + i) * LEVELS + 2 * z + l if 2 * z + l < LEVELS else None
                    for i in range(count)
                    for l in range(2)
                ],
            )
        if slot == 0:
            pl.when(early)(meet)
        if slot == slots - 1:
            spread(ws_ref[...])
            multiply(upper_levels, tok_levels)
            merge(0, [VARS_UP * LEVELS + v for v in range(VARS_SF)])

        @pl.when(jnp.logical_not(left_open))
        def _():
            for i in range(count):
                take_upper(t + i)
            if slot == slots - 1:
                take_surface()

        for low_range, high_range in sends[slot]:
            serve(low_range, high_range)
    pack_into(got_ref, me, me)

    def unpack(i, source):
        rows = got_ref[source].astype(jnp.float32)
        wide_ref[i] = rows
        main, raw = rows[:main_rows], rows[main_rows:]
        count = pad_rows - main_rows
        tail = jnp.zeros((count, 128), jnp.float32)
        for c in range(3):
            part = wide_ref[i, c * extra_rows : c * extra_rows + count]
            part = pltpu.roll(part, 128 - TO_SPARE[c], 1)
            tail = jnp.where(chunk_lanes(count, c), part, tail)
        if i == GROUP - 1:
            is_open = rows_of(source)
            tail = jnp.where(is_open, raw, tail)
            main = jnp.where(own_lanes(main_rows) | is_open, main, 0.0)
        return jnp.concatenate([main, tail], axis=0).astype(jnp.bfloat16)

    def gather(k, carry):
        g = partner(me // GROUP, k, groups)

        def wait_one(i, inner):
            source = g * GROUP + i

            @pl.when(source != me)
            def _():
                either(rows_of(source), lambda rows: copy_of(source, source, rows).wait_recv())

            return inner

        lax.fori_loop(0, GROUP, wait_one, 0)
        stacked = jnp.concatenate(
            [unpack(i, g * GROUP + i) for i in range(GROUP)], axis=1
        )
        moved = jnp.dot(stacked, place_ref[...], preferred_element_type=jnp.float32)
        start = g * (GROUP * pitch) + (lons - PATCH // 2)
        shift = lax.rem(start, 128)
        tile = lax.rem(start // 128, tiles)
        after = lax.rem(tile + 1, tiles)
        first_part = lane_of_pad >= shift
        for m in range(members):
            for q in range(PATCH):
                at = (m * PATCH + q) * 128
                value = pltpu.roll(moved[:, at : at + 128], shift, 1)
                rows = pl.ds(q, pad_rows, stride=PATCH)
                image_ref[m, tile, rows, :] += jnp.where(first_part, value, 0.0)
                image_ref[m, after, rows, :] += jnp.where(first_part, 0.0, value)
        return carry

    lane_of_pad = lax.broadcasted_iota(jnp.int32, (pad_rows, 128), 1)
    lax.fori_loop(0, groups, gather, 0)

    begin = 0 if own_rows % PATCH == 0 else lax.rem(me * own_rows, PATCH)
    for m in range(members):
        for tile in range(tiles):
            rows = image_ref[m, tile, pl.ds(begin, own_rows), :]
            out_ref[m, :, tile * 128 : (tile + 1) * 128] = rows.astype(jnp.bfloat16)

    def sent(r, carry):
        other = partner(me, r, windows)
        either(right_open, lambda rows: copy_of(me, other, rows).wait_send())
        return carry

    lax.fori_loop(1, windows, sent, 0)

    @pl.when(jnp.logical_not(right_open))
    def _():
        for index in range(up_tiles):
            edge_copy(index, edge_rows).wait_send()
        edge_copy(up_tiles, sf_tiles * part_rows).wait_send()


def tile_order(tiles):
    return (tiles - 2, 0, 2), (0, tiles - 2, 2)


def ranges_of(owners):
    ranges = []
    for o in owners:
        if ranges and ranges[-1][1] == o:
            ranges[-1][1] = o + 1
        else:
            ranges.append([o, o + 1])
    return ranges


def plan_of(spans, lat_rows, tiles):
    owners, depth = len(spans), LEVELS * lat_rows
    half, slots = owners // 2, -(-tiles // 2)
    sides = []
    for first, own in zip(tile_order(tiles), (range(half), range(half, owners))):
        done, sent, fresh = set(), set(), []
        for slot in range(slots):
            for t in range(first[slot], first[slot] + min(2, tiles - 2 * slot)):
                done.update(range(t * depth, (t + 1) * depth))
            if slot == slots - 1:
                done.update(range(tiles * depth, spans[-1][1]))
            new = [
                o for o in range(owners) if o not in sent and done.issuperset(range(*spans[o]))
            ]
            sent.update(new)
            fresh.append(([o for o in new if o in own], [o for o in new if o not in own]))
        sides.append(fresh)

    def both(slot, far):
        low, high = (ranges_of(side[slot][far]) for side in sides)
        count = max(len(low), len(high))
        low, high = (x + [[0, 0]] * (count - len(x)) for x in (low, high))
        return list(zip(low, high))

    return [both(0, 1) + both(0, 0)] + [both(slot, 0) + both(slot, 1) for slot in range(1, slots)]


def body(tokens, w_upper, w_surface, bias):
    members, tok_levels, lat_rows, lon_cols, width = tokens.shape
    windows = lax.axis_size("win")
    own_rows = CHANNELS * lat_rows * PATCH // windows
    lons = windows * lon_cols * PATCH
    spans = spans_of(windows, own_rows)
    longest = max(hi - lo for lo, hi in spans)
    main_rows = -(-3 * longest // 32) * 8
    extra_rows = max(longest - main_rows, 1)
    pad_rows = -(-longest // 16) * 16
    frame_rows = -(-(spans[-1][0] + pad_rows) // 8) * 8
    sends = plan_of(spans, lat_rows, w_upper.shape[1] // 128)
    edges = w_upper.shape[1] // 128 + 1
    bf16, f32 = jnp.bfloat16, jnp.float32
    by_lon = jnp.transpose(tokens, (0, 1, 3, 2, 4))
    return pl.pallas_call(
        functools.partial(kernel, (own_rows, main_rows, extra_rows, sends)),
        out_shape=pltpu.VMEM((members, own_rows, lons), bf16),
        in_specs=[pl.BlockSpec(memory_space=pltpu.HBM)] * 3
        + [pl.BlockSpec(memory_space=pltpu.SMEM)],
        out_specs=pl.BlockSpec(memory_space=pltpu.VMEM),
        scratch_shapes=[
            pltpu.VMEM(by_lon.shape, bf16),
            pltpu.VMEM(w_upper.shape, bf16),
            pltpu.VMEM(w_surface.shape, bf16),
            pltpu.VMEM((2, 2 * width, 256), bf16),
            pltpu.VMEM((members, 2, (tok_levels - 1) * lat_rows, 256), f32),
            pltpu.VMEM((frame_rows, 128), f32),
            pltpu.VMEM((windows, pad_rows, 128), bf16),
            pltpu.VMEM((windows, pad_rows, 128), bf16),
            pltpu.VMEM((edges, (tok_levels - 1) * lat_rows // 2, 128), bf16),
            pltpu.VMEM((edges, (tok_levels - 1) * lat_rows // 2, 128), bf16),
            pltpu.VMEM((128, 4 * 128), bf16),
            pltpu.VMEM((256, 1024), bf16),
            pltpu.VMEM((512, 256), bf16),
            pltpu.VMEM((GROUP * 128, members * PATCH * 128), bf16),
            pltpu.VMEM((members, lons // 128, pad_rows * PATCH, 128), f32),
            pltpu.VMEM((GROUP, pad_rows, 128), f32),
            pltpu.SemaphoreType.DMA((4,)),
            pltpu.SemaphoreType.DMA((windows,)),
            pltpu.SemaphoreType.DMA((windows,)),
            pltpu.SemaphoreType.DMA((2, edges)),
        ],
        compiler_params=pltpu.CompilerParams(
            collective_id=0, has_side_effects=True, vmem_limit_bytes=65 * 1000 * 1000
        ),
    )(by_lon, w_upper, w_surface, bias)


def solution(mesh):
    placed = (P("grp", None, None, "win", None), P(), P(), P())
    return jax.shard_map(
        body, mesh=mesh, in_specs=placed, out_specs=P("grp", "win", None), check_vma=False
    )
```

```python
import functools

import jax
import jax.numpy as jnp
from jax import lax
from jax.experimental import pallas as pl
from jax.experimental.pallas import tpu as pltpu
from jax.sharding import PartitionSpec as P

VARS_UP = 5
LEVELS = 13
VARS_SF = 4
PATCH = 4
GROUP = 8
TO_SPARE = (36, 32, 4)
CHANNELS = VARS_UP * LEVELS + VARS_SF


def spans_of(owners, own_rows):
    return [
        (o * own_rows // PATCH, -(-(o + 1) * own_rows // PATCH)) for o in range(owners)
    ]


def place_of(lane):
    return lane // 8 % 4, lane // 32 % 2 * 8 + lane % 8


def partner(me, r, windows):
    if windows & (windows - 1):
        return lax.rem(me + r, windows)
    return me ^ r


def kernel(
    plan, tok_hbm, wu_hbm, ws_hbm, bias_ref, out_ref,
    tok_ref, wu_ref, ws_ref, wb_ref, proj_ref, frame_ref, wire_ref, got_ref, edge_ref, side_ref, spot_ref,
    sel_ref, pick_ref,    place_ref, image_ref, wide_ref, load_sem, send_sem, recv_sem, edge_sem,
):
    members, tok_levels, lon_cols, lat_rows, width = tok_ref.shape
    windows, pad_rows, _ = wire_ref.shape
    half = windows // 2
    upper_levels = tok_levels - 1
    up_tiles = wu_ref.shape[1] // 128
    sf_tiles = ws_ref.shape[1] // 128
    me = lax.axis_index("win")
    own_rows, main_rows, extra_rows, sends = plan

    last = lon_cols - 1
    loads = [
        pltpu.make_async_copy(wu_hbm, wu_ref, load_sem.at[0]),
        pltpu.make_async_copy(ws_hbm, ws_ref, load_sem.at[1]),
        pltpu.make_async_copy(tok_hbm.at[:, :, last], tok_ref.at[:, :, last], load_sem.at[2]),
        pltpu.make_async_copy(
            tok_hbm.at[:, :, 0:last], tok_ref.at[:, :, 0:last], load_sem.at[3]
        ),
    ]
    for load in loads:
        load.start()

    barrier = pltpu.get_barrier_semaphore()

    def greet(r, carry):
        pl.semaphore_signal(
            barrier, inc=1, device_id={"win": partner(me, r, windows)},
            device_id_type=pl.DeviceIdType.MESH,
        )
        return carry

    lax.fori_loop(1, windows, greet, 0)

    def iota(shape, axis):
        return lax.broadcasted_iota(jnp.int32, shape, axis)

    def one_hot(hit):
        return jnp.where(hit, 1.0, 0.0).astype(jnp.bfloat16)

    def second_of(lat, half):
        return (lat + 2 + 4 * half) % 8

    def source_of(tile, level, lat, lon):
        return tile * 128 + level * 64 + lat * 8 + lon

    for side in range(2):
        for near in range(2):
            row = iota((256, 256), 0)
            n = iota((256, 256), 1)
            k = side * 8 + n % 8 - PATCH * (side + near)
            lat = second_of(n // 8 % 4, n // 128)
            hit = row == source_of(n // 64 % 2, n // 32 % 2, lat, k)
            at = (2 * side + near) * 256
            sel_ref[:, at : at + 256] = one_hot(hit & (k >= 0) & (k < 2 * PATCH))
    row = iota(pick_ref.shape, 0)
    n = iota(pick_ref.shape, 1)
    lat = second_of(n // 4 % 4, n // 128)
    pick_ref[...] = one_hot(row == source_of(n // 32 % 4, n // 16 % 2, lat, n % 4 + PATCH))
    row = iota(spot_ref.shape, 0)
    n = iota(spot_ref.shape, 1)
    to_lane = row // 64 * 64 + row // 4 % 4 * 8 + row % 4
    spot_ref[...] = one_hot(n == row // 16 % 4 * 128 + to_lane)

    def spread(w):
        wide = jnp.dot(w, sel_ref[0 : w.shape[1], :], preferred_element_type=jnp.float32)
        for side in range(2):
            for near in range(2):
                at = (2 * side + near) * 256
                wb_ref[side, near * width : (near + 1) * width, :] = wide[
                    :, at : at + 256
                ].astype(jnp.bfloat16)

    lane = iota((lat_rows, 128), 1)
    line = iota((lat_rows, 128), 0)
    frame_lower = lane % 32 < 16
    edge_lower = lane % 16 < 8
    own_lane = place_of(lane)[1] < 12

    def own_lanes(rows):
        return place_of(iota((rows, 128), 1))[1] < 12

    def chunk_lanes(rows, c):
        return place_of(iota((rows, 128), 1))[1] // 4 == c

    def image(y, lower):
        first, second = y[:, :128], y[:, 128:]
        moved = jnp.where(
            lower, pltpu.roll(second, 1, 0), pltpu.roll(second, lat_rows - 1, 0)
        )
        keep = line != jnp.where(lower, 0, lat_rows - 1)
        return first + jnp.where(keep, moved, 0.0)

    def exchange(parts, wanted):
        at = iota(parts[0].shape, 1)
        low_half, even = at < 64, at // 32 % 2 == 0
        halves = []
        for h in range(-(-wanted // 2)):
            for a, b in ((parts[0], parts[2]), (parts[1], parts[3])):
                if h == 0:
                    halves.append(jnp.where(low_half, a, pltpu.roll(b, 64, 1)))
                else:
                    halves.append(jnp.where(low_half, pltpu.roll(a, 64, 1), b))
        out = []
        for p in range(wanted):
            a, b = halves[p // 2 * 2], halves[p // 2 * 2 + 1]
            if p % 2 == 0:
                out.append(jnp.where(even, a, pltpu.roll(b, 32, 1)))
            else:
                out.append(jnp.where(even, pltpu.roll(a, 96, 1), b))
        return out

    def put(channel, block):
        start = pl.multiple_of(channel * lat_rows, 8)
        frame_ref[pl.ds(start, lat_rows), :] = block + jnp.where(own_lane, bias_ref[channel], 0.0)

    def multiply(z0, z1):
        rows = (z1 - z0) * lat_rows
        for m in range(members):
            token = [tok_ref[m, z0:z1, j].reshape(rows, width) for j in range(lon_cols)]
            for side in range(2):
                proj_ref[m, side, 0:rows] = jnp.dot(
                    jnp.concatenate(token[side : side + 2], axis=1), wb_ref[side],
                    preferred_element_type=jnp.float32,
                )

    def merge(z, channels):
        at = slice(z * lat_rows, (z + 1) * lat_rows)
        parts = [
            image(proj_ref[m, side, at, :], frame_lower)
            for m in range(members)
            for side in range(2)
        ]
        for channel, block in zip(channels, exchange(parts, len(channels))):
            if channel is not None:
                put(channel, block)

    low = me < half

    def first_tile(slot):
        low_tiles, high_tiles = tile_order(up_tiles)
        return jnp.where(low, low_tiles[slot], high_tiles[slot])

    def tiles_of(slot):
        return min(2, up_tiles - 2 * slot)

    left_open = lax.rem(me, half) == 0
    right_open = lax.rem(me + 1, half) == 0

    def edge_copy(index, rows):
        return pltpu.make_async_remote_copy(
            src_ref=edge_ref.at[index, 0:rows],
            dst_ref=side_ref.at[index, 0:rows],
            send_sem=edge_sem.at[0, index],
            recv_sem=edge_sem.at[1, index],
            device_id={"win": lax.rem(me + 1, windows)},
            device_id_type=pl.DeviceIdType.MESH,
        )

    part_rows = lat_rows // 2
    edge_rows = upper_levels * part_rows

    def edges(w, z0, z1, put_edge):
        rows = (z1 - z0) * lat_rows
        weights = jnp.dot(w, pick_ref[0 : w.shape[1], :], preferred_element_type=jnp.float32)
        weights = weights.astype(jnp.bfloat16)
        for m in range(members):
            proj_ref[m, 0, 0:rows] = jnp.dot(
                tok_ref[m, z0:z1, last].reshape(rows, width), weights,
                preferred_element_type=jnp.float32,
            )
        for z in range(z1 - z0):
            parts = []
            for m in range(members):
                x = image(proj_ref[m, 0, z * lat_rows : (z + 1) * lat_rows, :], edge_lower)
                parts += [x[:part_rows], x[part_rows:]]
            for i, block in enumerate(exchange(parts, w.shape[1] // 128)):
                put_edge(i, z, block.astype(jnp.bfloat16))

    def make_edges():
        for load in loads[:3]:
            load.wait()
        for v in range(0, up_tiles, 4):

            def put_upper(i, z, block):
                edge_ref[v + i, z * part_rows : (z + 1) * part_rows] = block

            edges(wu_ref[:, v * 128 : min(v + 4, up_tiles) * 128], 0, upper_levels, put_upper)

        def put_surface(i, z, block):
            edge_ref[up_tiles, i * part_rows : (i + 1) * part_rows] = block

        edges(ws_ref[...], upper_levels, tok_levels, put_surface)

    def send_edges():
        @pl.when(jnp.logical_not(right_open))
        def _():
            for slot in range(slots):
                for i in range(tiles_of(slot)):
                    edge_copy(first_tile(slot) + i, edge_rows).start()
                if slot == slots - 1:
                    edge_copy(up_tiles, sf_tiles * part_rows).start()

    def take_edge(index, rows):
        edge_copy(index, rows).wait_recv()
        return jnp.dot(
            side_ref[index, 0:rows], spot_ref[...], preferred_element_type=jnp.float32
        )

    def add_rows(channel, h, block):
        at = pl.multiple_of(channel * lat_rows + h * part_rows, 8)
        frame_ref[pl.ds(at, part_rows), :] += block

    def take_upper(t):
        moved = take_edge(t, edge_rows)
        for z in range(upper_levels):
            for h in range(2):
                for l in range(min(2, LEVELS - 2 * z)):
                    lanes = (2 * h + l) * 128
                    block = moved[z * part_rows : (z + 1) * part_rows, lanes : lanes + 128]
                    add_rows(t * LEVELS + 2 * z + l, h, block)

    def take_surface():
        moved = take_edge(up_tiles, sf_tiles * part_rows)
        for i in range(sf_tiles):
            for h in range(2):
                for l in range(2):
                    lanes = (2 * h + l) * 128
                    block = moved[i * part_rows : (i + 1) * part_rows, lanes : lanes + 128]
                    add_rows(VARS_UP * LEVELS + 2 * i + l, h, block)

    def rows_of(window):
        return lax.rem(window + 1, half) == 0

    def copy_of(source, other, rows):
        return pltpu.make_async_remote_copy(
            src_ref=wire_ref.at[other, 0:rows],
            dst_ref=got_ref.at[source, 0:rows],
            send_sem=send_sem.at[other],
            recv_sem=recv_sem.at[source],
            device_id={"win": other},
            device_id_type=pl.DeviceIdType.MESH,
        )

    def either(is_open, run):
        @pl.when(is_open)
        def _():
            run(pad_rows)

        @pl.when(jnp.logical_not(is_open))
        def _():
            run(main_rows)

    def pack_into(ref, index, other):
        start = other * own_rows // PATCH
        main = frame_ref[pl.ds(start, main_rows), :]
        tail = frame_ref[pl.ds(start + main_rows, pad_rows - main_rows), :]
        chunks = []
        for c in range(3):
            first = c * extra_rows // 8 * 8
            end = min(-(-(c + 1) * extra_rows // 8) * 8, main_rows) if c < 2 else main_rows
            rows = frame_ref[pl.ds(start + main_rows - c * extra_rows + first, end - first), :]
            chunks.append((first, pltpu.roll(rows, TO_SPARE[c], 1)))
        line_of_8 = iota((8, 128), 0)
        spare = []
        for at in range(0, main_rows, 8):
            block = None
            for c, (first, rows) in enumerate(chunks):
                if first <= at < first + rows.shape[0]:
                    part = rows[at - first : at - first + 8]
                    begins = line_of_8 >= c * extra_rows - at
                    block = part if block is None else jnp.where(begins, part, block)
            spare.append(block)
        kept = own_lanes(main_rows) | right_open
        main = jnp.where(kept, main, jnp.concatenate(spare, axis=0))
        ref[index] = jnp.concatenate([main, tail], axis=0).astype(jnp.bfloat16)

    pair_of_me = me // 2

    def serve(low_range, high_range, near):
        begin, end = (jnp.where(low, a, b) for a, b in zip(low_range, high_range))
        first_pair = begin // 2
        pairs = (end + 1) // 2 - first_pair

        def send(i, carry):
            pair = first_pair + lax.rem(i + pair_of_me, jnp.maximum(pairs, 1))
            wanted = True if near is None else (lax.rem(pair // 2, 2) == lax.rem(pair_of_me // 2, 2)) == near

            @pl.when(wanted)
            def _():
                one, two = 2 * pair, 2 * pair + 1
                first, second = jnp.maximum(one, begin), jnp.minimum(two, end - 1)
                pack_into(wire_ref, first, first)
                pack_into(wire_ref, second, second)

                @pl.when((one != me) & (one >= begin))
                def _():
                    either(right_open, lambda rows: copy_of(me, one, rows).start())

                @pl.when((two != me) & (two < end))
                def _():
                    either(right_open, lambda rows: copy_of(me, two, rows).start())

            return carry

        lax.fori_loop(0, pairs, send, 0)

    slots = -(-up_tiles // 2)
    tiles = image_ref.shape[1]
    lons = tiles * 128
    groups = windows // GROUP
    pitch = lons // windows
    row = iota((128, place_ref.shape[1]), 0)
    col = iota(row.shape, 1)
    row_q, row_column = place_of(row)
    target = row // 64 * 512 + row_q * 128 + row_column

    def fill(i, carry):
        hit = (col == target + i * pitch) & ((row_column < 12) | (i == GROUP - 1))
        place_ref[pl.ds(pl.multiple_of(i * 128, 128), 128), :] = one_hot(hit)
        return carry

    lax.fori_loop(0, GROUP, fill, 0)
    image_ref[...] = jnp.zeros(image_ref.shape, jnp.float32)
    frame_ref[...] = jnp.zeros(frame_ref.shape, jnp.float32)
    def spread_upper(slot):
        t, count = first_tile(slot), tiles_of(slot)
        spread(wu_ref[:, pl.ds(pl.multiple_of(t * 128, 128), count * 128)])

    def meet():
        pl.semaphore_wait(barrier, windows - 1)
        send_edges()

    def settle(slot):
        @pl.when(jnp.logical_not(left_open))
        def _():
            for i in range(tiles_of(slot)):
                take_upper(first_tile(slot) + i)
            if slot == slots - 1:
                take_surface()

        for low_range, high_range, near in sends[slot]:
            serve(low_range, high_range, near)

    make_edges()
    spread_upper(0)
    early = me < windows // 4
    earliest = me < windows // 16
    pl.when(jnp.logical_not(early))(meet)
    loads[3].wait()
    for slot in range(slots):
        t, count = first_tile(slot), tiles_of(slot)
        if slot > 0:
            spread_upper(slot)
        multiply(0, upper_levels)
        for z in range(upper_levels):
            merge(
                z,
                [
                    (t + i) * LEVELS + 2 * z + l if 2 * z + l < LEVELS else None
                    for i in range(count)
                    for l in range(2)
                ],
            )
        if slot == slots - 1:
            spread(ws_ref[...])
            multiply(upper_levels, tok_levels)
            merge(0, [VARS_UP * LEVELS + v for v in range(VARS_SF)])

        if slot == 0:
            pl.when(early & jnp.logical_not(earliest))(meet)
            pl.when(jnp.logical_not(earliest))(functools.partial(settle, 0))
        else:
            if slot == 1:

                @pl.when(earliest)
                def _():
                    meet()
                    settle(0)

            settle(slot)
    pack_into(got_ref, me, me)

    def unpack(i, source):
        rows = got_ref[source].astype(jnp.float32)
        wide_ref[i] = rows
        main, raw = rows[:main_rows], rows[main_rows:]
        count = pad_rows - main_rows
        tail = jnp.zeros((count, 128), jnp.float32)
        for c in range(3):
            part = wide_ref[i, c * extra_rows : c * extra_rows + count]
            part = pltpu.roll(part, 128 - TO_SPARE[c], 1)
            tail = jnp.where(chunk_lanes(count, c), part, tail)
        if i == GROUP - 1:
            is_open = rows_of(source)
            tail = jnp.where(is_open, raw, tail)
            main = jnp.where(own_lanes(main_rows) | is_open, main, 0.0)
        return jnp.concatenate([main, tail], axis=0).astype(jnp.bfloat16)

    def gather(k, carry):
        g = partner(me // GROUP, k, groups)

        def wait_one(i, inner):
            source = g * GROUP + i

            @pl.when(source != me)
            def _():
                either(rows_of(source), lambda rows: copy_of(source, source, rows).wait_recv())

            return inner

        lax.fori_loop(0, GROUP, wait_one, 0)
        stacked = jnp.concatenate(
            [unpack(i, g * GROUP + i) for i in range(GROUP)], axis=1
        )
        moved = jnp.dot(stacked, place_ref[...], preferred_element_type=jnp.float32)
        start = g * (GROUP * pitch) + (lons - PATCH // 2)
        shift = lax.rem(start, 128)
        tile = lax.rem(start // 128, tiles)
        after = lax.rem(tile + 1, tiles)
        first_part = lane_of_pad >= shift
        for m in range(members):
            for q in range(PATCH):
                at = (m * PATCH + q) * 128
                value = pltpu.roll(moved[:, at : at + 128], shift, 1)
                rows = pl.ds(q, pad_rows, stride=PATCH)
                image_ref[m, tile, rows, :] += jnp.where(first_part, value, 0.0)
                image_ref[m, after, rows, :] += jnp.where(first_part, 0.0, value)
        return carry

    lane_of_pad = lax.broadcasted_iota(jnp.int32, (pad_rows, 128), 1)
    lax.fori_loop(0, groups, gather, 0)

    begin = 0 if own_rows % PATCH == 0 else lax.rem(me * own_rows, PATCH)
    for m in range(members):
        for tile in range(tiles):
            rows = image_ref[m, tile, pl.ds(begin, own_rows), :]
            out_ref[m, :, tile * 128 : (tile + 1) * 128] = rows.astype(jnp.bfloat16)

    def sent(r, carry):
        other = partner(me, r, windows)
        either(right_open, lambda rows: copy_of(me, other, rows).wait_send())
        return carry

    lax.fori_loop(1, windows, sent, 0)

    @pl.when(jnp.logical_not(right_open))
    def _():
        for index in range(up_tiles):
            edge_copy(index, edge_rows).wait_send()
        edge_copy(up_tiles, sf_tiles * part_rows).wait_send()


def tile_order(tiles):
    return (tiles - 2, 0, 2), (0, tiles - 2, 2)


def ranges_of(owners):
    ranges = []
    for o in owners:
        if ranges and ranges[-1][1] == o:
            ranges[-1][1] = o + 1
        else:
            ranges.append([o, o + 1])
    return ranges


def plan_of(spans, lat_rows, tiles):
    owners, depth = len(spans), LEVELS * lat_rows
    half, slots = owners // 2, -(-tiles // 2)
    sides = []
    for first, own in zip(tile_order(tiles), (range(half), range(half, owners))):
        done, sent, fresh = set(), set(), []
        for slot in range(slots):
            for t in range(first[slot], first[slot] + min(2, tiles - 2 * slot)):
                done.update(range(t * depth, (t + 1) * depth))
            if slot == slots - 1:
                done.update(range(tiles * depth, spans[-1][1]))
            new = [
                o for o in range(owners) if o not in sent and done.issuperset(range(*spans[o]))
            ]
            sent.update(new)
            fresh.append(([o for o in new if o in own], [o for o in new if o not in own]))
        sides.append(fresh)

    def both(slot, far, near):
        low, high = (ranges_of(side[slot][far]) for side in sides)
        count = max(len(low), len(high))
        low, high = (x + [[0, 0]] * (count - len(x)) for x in (low, high))
        return [(a, b, near) for a, b in zip(low, high)]

    sends = [both(0, 1, True)]
    for slot in range(1, slots):
        now = both(0, 0, None) if slot == 1 else []
        now += both(slot, 0, None)
        now += both(0, 1, False) if slot == 1 else []
        sends.append(now + both(slot, 1, None))
    return sends


def body(tokens, w_upper, w_surface, bias):
    members, tok_levels, lat_rows, lon_cols, width = tokens.shape
    windows = lax.axis_size("win")
    own_rows = CHANNELS * lat_rows * PATCH // windows
    lons = windows * lon_cols * PATCH
    spans = spans_of(windows, own_rows)
    longest = max(hi - lo for lo, hi in spans)
    main_rows = -(-3 * longest // 32) * 8
    extra_rows = max(longest - main_rows, 1)
    pad_rows = -(-longest // 16) * 16
    frame_rows = -(-(spans[-1][0] + pad_rows) // 8) * 8
    sends = plan_of(spans, lat_rows, w_upper.shape[1] // 128)
    edges = w_upper.shape[1] // 128 + 1
    bf16, f32 = jnp.bfloat16, jnp.float32
    by_lon = jnp.transpose(tokens, (0, 1, 3, 2, 4))
    return pl.pallas_call(
        functools.partial(kernel, (own_rows, main_rows, extra_rows, sends)),
        out_shape=pltpu.VMEM((members, own_rows, lons), bf16),
        in_specs=[pl.BlockSpec(memory_space=pltpu.HBM)] * 3
        + [pl.BlockSpec(memory_space=pltpu.SMEM)],
        out_specs=pl.BlockSpec(memory_space=pltpu.VMEM),
        scratch_shapes=[
            pltpu.VMEM(by_lon.shape, bf16),
            pltpu.VMEM(w_upper.shape, bf16),
            pltpu.VMEM(w_surface.shape, bf16),
            pltpu.VMEM((2, 2 * width, 256), bf16),
            pltpu.VMEM((members, 2, (tok_levels - 1) * lat_rows, 256), f32),
            pltpu.VMEM((frame_rows, 128), f32),
            pltpu.VMEM((windows, pad_rows, 128), bf16),
            pltpu.VMEM((windows, pad_rows, 128), bf16),
            pltpu.VMEM((edges, (tok_levels - 1) * lat_rows // 2, 128), bf16),
            pltpu.VMEM((edges, (tok_levels - 1) * lat_rows // 2, 128), bf16),
            pltpu.VMEM((128, 4 * 128), bf16),
            pltpu.VMEM((256, 1024), bf16),
            pltpu.VMEM((512, 256), bf16),
            pltpu.VMEM((GROUP * 128, members * PATCH * 128), bf16),
            pltpu.VMEM((members, lons // 128, pad_rows * PATCH, 128), f32),
            pltpu.VMEM((GROUP, pad_rows, 128), f32),
            pltpu.SemaphoreType.DMA((4,)),
            pltpu.SemaphoreType.DMA((windows,)),
            pltpu.SemaphoreType.DMA((windows,)),
            pltpu.SemaphoreType.DMA((2, edges)),
        ],
        compiler_params=pltpu.CompilerParams(
            collective_id=0, has_side_effects=True, vmem_limit_bytes=65 * 1000 * 1000
        ),
    )(by_lon, w_upper, w_surface, bias)


def solution(mesh):
    placed = (P("grp", None, None, "win", None), P(), P(), P())
    return jax.shard_map(
        body, mesh=mesh, in_specs=placed, out_specs=P("grp", "win", None), check_vma=False
    )
```

```python
import functools

import jax
import jax.numpy as jnp
from jax import lax
from jax.experimental import pallas as pl
from jax.experimental.pallas import tpu as pltpu
from jax.sharding import PartitionSpec as P

VARS_UP = 5
LEVELS = 13
VARS_SF = 4
PATCH = 4
GROUP = 8
TO_SPARE = (36, 32, 4)
CHANNELS = VARS_UP * LEVELS + VARS_SF


def spans_of(owners, own_rows):
    return [
        (o * own_rows // PATCH, -(-(o + 1) * own_rows // PATCH)) for o in range(owners)
    ]


def place_of(lane):
    return lane // 8 % 4, lane // 32 % 2 * 8 + lane % 8


def partner(me, r, windows):
    if windows & (windows - 1):
        return lax.rem(me + r, windows)
    return me ^ r


def kernel(
    plan, tok_hbm, wu_hbm, ws_hbm, bias_ref, out_ref,
    tok_ref, wu_ref, ws_ref, wb_ref, proj_ref, frame_ref, wire_ref, got_ref, edge_ref, side_ref, spot_ref,
    sel_ref, pick_ref,    place_ref, image_ref, wide_ref, load_sem, send_sem, recv_sem, edge_sem,
):
    members, tok_levels, lon_cols, lat_rows, width = tok_ref.shape
    windows, pad_rows, _ = wire_ref.shape
    half = windows // 2
    upper_levels = tok_levels - 1
    up_tiles = wu_ref.shape[1] // 128
    sf_tiles = ws_ref.shape[1] // 128
    me = lax.axis_index("win")
    own_rows, main_rows, extra_rows, sends = plan

    last = lon_cols - 1
    loads = [
        pltpu.make_async_copy(wu_hbm, wu_ref, load_sem.at[0]),
        pltpu.make_async_copy(ws_hbm, ws_ref, load_sem.at[1]),
        pltpu.make_async_copy(tok_hbm.at[:, :, last], tok_ref.at[:, :, last], load_sem.at[2]),
        pltpu.make_async_copy(
            tok_hbm.at[:, :, 0:last], tok_ref.at[:, :, 0:last], load_sem.at[3]
        ),
    ]
    for load in loads:
        load.start()

    barrier = pltpu.get_barrier_semaphore()

    def greet(r, carry):
        pl.semaphore_signal(
            barrier, inc=1, device_id={"win": partner(me, windows - r, windows)},
            device_id_type=pl.DeviceIdType.MESH,
        )
        return carry

    lax.fori_loop(1, windows, greet, 0)

    def iota(shape, axis):
        return lax.broadcasted_iota(jnp.int32, shape, axis)

    def one_hot(hit):
        return jnp.where(hit, 1.0, 0.0).astype(jnp.bfloat16)

    def second_of(lat, half):
        return (lat + 2 + 4 * half) % 8

    def source_of(tile, level, lat, lon):
        return tile * 128 + level * 64 + lat * 8 + lon

    for side in range(2):
        for near in range(2):
            row = iota((256, 256), 0)
            n = iota((256, 256), 1)
            k = side * 8 + n % 8 - PATCH * (side + near)
            lat = second_of(n // 8 % 4, n // 128)
            hit = row == source_of(n // 64 % 2, n // 32 % 2, lat, k)
            at = (2 * side + near) * 256
            sel_ref[:, at : at + 256] = one_hot(hit & (k >= 0) & (k < 2 * PATCH))
    row = iota(pick_ref.shape, 0)
    n = iota(pick_ref.shape, 1)
    lat = second_of(n // 4 % 4, n // 128)
    pick_ref[...] = one_hot(row == source_of(n // 32 % 4, n // 16 % 2, lat, n % 4 + PATCH))
    row = iota(spot_ref.shape, 0)
    n = iota(spot_ref.shape, 1)
    to_lane = row // 64 * 64 + row // 4 % 4 * 8 + row % 4
    spot_ref[...] = one_hot(n == row // 16 % 4 * 128 + to_lane)

    def spread(w):
        wide = jnp.dot(w, sel_ref[0 : w.shape[1], :], preferred_element_type=jnp.float32)
        for side in range(2):
            for near in range(2):
                at = (2 * side + near) * 256
                wb_ref[side, near * width : (near + 1) * width, :] = wide[
                    :, at : at + 256
                ].astype(jnp.bfloat16)

    lane = iota((lat_rows, 128), 1)
    line = iota((lat_rows, 128), 0)
    frame_lower = lane % 32 < 16
    edge_lower = lane % 16 < 8
    own_lane = place_of(lane)[1] < 12

    def own_lanes(rows):
        return place_of(iota((rows, 128), 1))[1] < 12

    def chunk_lanes(rows, c):
        return place_of(iota((rows, 128), 1))[1] // 4 == c

    def image(y, lower):
        first, second = y[:, :128], y[:, 128:]
        moved = jnp.where(
            lower, pltpu.roll(second, 1, 0), pltpu.roll(second, lat_rows - 1, 0)
        )
        keep = line != jnp.where(lower, 0, lat_rows - 1)
        return first + jnp.where(keep, moved, 0.0)

    def exchange(parts, wanted):
        at = iota(parts[0].shape, 1)
        low_half, even = at < 64, at // 32 % 2 == 0
        halves = []
        for h in range(-(-wanted // 2)):
            for a, b in ((parts[0], parts[2]), (parts[1], parts[3])):
                if h == 0:
                    halves.append(jnp.where(low_half, a, pltpu.roll(b, 64, 1)))
                else:
                    halves.append(jnp.where(low_half, pltpu.roll(a, 64, 1), b))
        out = []
        for p in range(wanted):
            a, b = halves[p // 2 * 2], halves[p // 2 * 2 + 1]
            if p % 2 == 0:
                out.append(jnp.where(even, a, pltpu.roll(b, 32, 1)))
            else:
                out.append(jnp.where(even, pltpu.roll(a, 96, 1), b))
        return out

    def put(channel, block):
        start = pl.multiple_of(channel * lat_rows, 8)
        frame_ref[pl.ds(start, lat_rows), :] = block + jnp.where(own_lane, bias_ref[channel], 0.0)

    def multiply(z0, z1):
        rows = (z1 - z0) * lat_rows
        for m in range(members):
            token = [tok_ref[m, z0:z1, j].reshape(rows, width) for j in range(lon_cols)]
            for side in range(2):
                proj_ref[m, side, 0:rows] = jnp.dot(
                    jnp.concatenate(token[side : side + 2], axis=1), wb_ref[side],
                    preferred_element_type=jnp.float32,
                )

    def merge(z, channels):
        at = slice(z * lat_rows, (z + 1) * lat_rows)
        parts = [
            image(proj_ref[m, side, at, :], frame_lower)
            for m in range(members)
            for side in range(2)
        ]
        for channel, block in zip(channels, exchange(parts, len(channels))):
            if channel is not None:
                put(channel, block)

    low = me < half

    def first_tile(slot):
        low_tiles, high_tiles = tile_order(up_tiles)
        return jnp.where(low, low_tiles[slot], high_tiles[slot])

    def tiles_of(slot):
        return min(2, up_tiles - 2 * slot)

    left_open = lax.rem(me, half) == 0
    right_open = lax.rem(me + 1, half) == 0

    def edge_copy(index, rows):
        return pltpu.make_async_remote_copy(
            src_ref=edge_ref.at[index, 0:rows],
            dst_ref=side_ref.at[index, 0:rows],
            send_sem=edge_sem.at[0, index],
            recv_sem=edge_sem.at[1, index],
            device_id={"win": lax.rem(me + 1, windows)},
            device_id_type=pl.DeviceIdType.MESH,
        )

    part_rows = lat_rows // 2
    edge_rows = upper_levels * part_rows

    def edges(w, z0, z1, put_edge):
        rows = (z1 - z0) * lat_rows
        weights = jnp.dot(w, pick_ref[0 : w.shape[1], :], preferred_element_type=jnp.float32)
        weights = weights.astype(jnp.bfloat16)
        for m in range(members):
            proj_ref[m, 0, 0:rows] = jnp.dot(
                tok_ref[m, z0:z1, last].reshape(rows, width), weights,
                preferred_element_type=jnp.float32,
            )
        for z in range(z1 - z0):
            parts = []
            for m in range(members):
                x = image(proj_ref[m, 0, z * lat_rows : (z + 1) * lat_rows, :], edge_lower)
                parts += [x[:part_rows], x[part_rows:]]
            for i, block in enumerate(exchange(parts, w.shape[1] // 128)):
                put_edge(i, z, block.astype(jnp.bfloat16))

    def make_edges():
        for load in loads[:3]:
            load.wait()
        for v in range(0, up_tiles, 4):

            def put_upper(i, z, block):
                edge_ref[v + i, z * part_rows : (z + 1) * part_rows] = block

            edges(wu_ref[:, v * 128 : min(v + 4, up_tiles) * 128], 0, upper_levels, put_upper)

        def put_surface(i, z, block):
            edge_ref[up_tiles, i * part_rows : (i + 1) * part_rows] = block

        edges(ws_ref[...], upper_levels, tok_levels, put_surface)

    def send_edges():
        @pl.when(jnp.logical_not(right_open))
        def _():
            for slot in range(slots):
                for i in range(tiles_of(slot)):
                    edge_copy(first_tile(slot) + i, edge_rows).start()
                if slot == slots - 1:
                    edge_copy(up_tiles, sf_tiles * part_rows).start()

    def take_edge(index, rows):
        edge_copy(index, rows).wait_recv()
        return jnp.dot(
            side_ref[index, 0:rows], spot_ref[...], preferred_element_type=jnp.float32
        )

    def add_rows(channel, h, block):
        at = pl.multiple_of(channel * lat_rows + h * part_rows, 8)
        frame_ref[pl.ds(at, part_rows), :] += block

    def take_upper(t):
        moved = take_edge(t, edge_rows)
        for z in range(upper_levels):
            for h in range(2):
                for l in range(min(2, LEVELS - 2 * z)):
                    lanes = (2 * h + l) * 128
                    block = moved[z * part_rows : (z + 1) * part_rows, lanes : lanes + 128]
                    add_rows(t * LEVELS + 2 * z + l, h, block)

    def take_surface():
        moved = take_edge(up_tiles, sf_tiles * part_rows)
        for i in range(sf_tiles):
            for h in range(2):
                for l in range(2):
                    lanes = (2 * h + l) * 128
                    block = moved[i * part_rows : (i + 1) * part_rows, lanes : lanes + 128]
                    add_rows(VARS_UP * LEVELS + 2 * i + l, h, block)

    def rows_of(window):
        return lax.rem(window + 1, half) == 0

    def copy_of(source, other, rows):
        return pltpu.make_async_remote_copy(
            src_ref=wire_ref.at[other, 0:rows],
            dst_ref=got_ref.at[source, 0:rows],
            send_sem=send_sem.at[other],
            recv_sem=recv_sem.at[source],
            device_id={"win": other},
            device_id_type=pl.DeviceIdType.MESH,
        )

    def either(is_open, run):
        @pl.when(is_open)
        def _():
            run(pad_rows)

        @pl.when(jnp.logical_not(is_open))
        def _():
            run(main_rows)

    def pack_into(ref, index, other):
        start = other * own_rows // PATCH
        main = frame_ref[pl.ds(start, main_rows), :]
        tail = frame_ref[pl.ds(start + main_rows, pad_rows - main_rows), :]
        chunks = []
        for c in range(3):
            first = c * extra_rows // 8 * 8
            end = min(-(-(c + 1) * extra_rows // 8) * 8, main_rows) if c < 2 else main_rows
            rows = frame_ref[pl.ds(start + main_rows - c * extra_rows + first, end - first), :]
            chunks.append((first, pltpu.roll(rows, TO_SPARE[c], 1)))
        line_of_8 = iota((8, 128), 0)
        spare = []
        for at in range(0, main_rows, 8):
            block = None
            for c, (first, rows) in enumerate(chunks):
                if first <= at < first + rows.shape[0]:
                    part = rows[at - first : at - first + 8]
                    begins = line_of_8 >= c * extra_rows - at
                    block = part if block is None else jnp.where(begins, part, block)
            spare.append(block)
        kept = own_lanes(main_rows) | right_open
        main = jnp.where(kept, main, jnp.concatenate(spare, axis=0))
        ref[index] = jnp.concatenate([main, tail], axis=0).astype(jnp.bfloat16)

    pair_of_me = me // 2

    def serve(low_range, high_range, near):
        begin, end = (jnp.where(low, a, b) for a, b in zip(low_range, high_range))
        first_pair = begin // 2
        pairs = (end + 1) // 2 - first_pair

        def send(i, carry):
            pair = first_pair + lax.rem(i + pair_of_me, jnp.maximum(pairs, 1))
            wanted = True if near is None else (lax.rem(pair // 2, 2) == lax.rem(pair_of_me // 2, 2)) == near

            @pl.when(wanted)
            def _():
                one, two = 2 * pair, 2 * pair + 1
                first, second = jnp.maximum(one, begin), jnp.minimum(two, end - 1)
                pack_into(wire_ref, first, first)
                pack_into(wire_ref, second, second)

                @pl.when((one != me) & (one >= begin))
                def _():
                    either(right_open, lambda rows: copy_of(me, one, rows).start())

                @pl.when((two != me) & (two < end))
                def _():
                    either(right_open, lambda rows: copy_of(me, two, rows).start())

            return carry

        lax.fori_loop(0, pairs, send, 0)

    slots = -(-up_tiles // 2)
    tiles = image_ref.shape[1]
    lons = tiles * 128
    groups = windows // GROUP
    pitch = lons // windows
    row = iota((128, place_ref.shape[1]), 0)
    col = iota(row.shape, 1)
    row_q, row_column = place_of(row)
    target = row // 64 * 512 + row_q * 128 + row_column

    def fill(i, carry):
        hit = (col == target + i * pitch) & ((row_column < 12) | (i == GROUP - 1))
        place_ref[pl.ds(pl.multiple_of(i * 128, 128), 128), :] = one_hot(hit)
        return carry

    lax.fori_loop(0, GROUP, fill, 0)
    image_ref[...] = jnp.zeros(image_ref.shape, jnp.float32)
    frame_ref[...] = jnp.zeros(frame_ref.shape, jnp.float32)
    def spread_upper(slot):
        t, count = first_tile(slot), tiles_of(slot)
        spread(wu_ref[:, pl.ds(pl.multiple_of(t * 128, 128), count * 128)])

    def meet():
        pl.semaphore_wait(barrier, windows - 1)
        send_edges()

    def settle(slot):
        @pl.when(jnp.logical_not(left_open))
        def _():
            for i in range(tiles_of(slot)):
                take_upper(first_tile(slot) + i)
            if slot == slots - 1:
                take_surface()

        for low_range, high_range, near in sends[slot]:
            serve(low_range, high_range, near)

    make_edges()
    spread_upper(0)
    early = me < windows // 4
    earliest = me < windows // 16
    pl.when(jnp.logical_not(early))(meet)
    loads[3].wait()
    for slot in range(slots):
        t, count = first_tile(slot), tiles_of(slot)
        if slot > 0:
            spread_upper(slot)
        multiply(0, upper_levels)
        for z in range(upper_levels):
            merge(
                z,
                [
                    (t + i) * LEVELS + 2 * z + l if 2 * z + l < LEVELS else None
                    for i in range(count)
                    for l in range(2)
                ],
            )
        if slot == slots - 1:
            spread(ws_ref[...])
            multiply(upper_levels, tok_levels)
            merge(0, [VARS_UP * LEVELS + v for v in range(VARS_SF)])

        if slot == 0:
            pl.when(early & jnp.logical_not(earliest))(meet)
            pl.when(jnp.logical_not(earliest))(functools.partial(settle, 0))
        else:
            if slot == 1:

                @pl.when(earliest)
                def _():
                    meet()
                    settle(0)

            settle(slot)
    pack_into(got_ref, me, me)

    def unpack(i, source):
        rows = got_ref[source].astype(jnp.float32)
        wide_ref[i] = rows
        main, raw = rows[:main_rows], rows[main_rows:]
        count = pad_rows - main_rows
        tail = jnp.zeros((count, 128), jnp.float32)
        for c in range(3):
            part = wide_ref[i, c * extra_rows : c * extra_rows + count]
            part = pltpu.roll(part, 128 - TO_SPARE[c], 1)
            tail = jnp.where(chunk_lanes(count, c), part, tail)
        if i == GROUP - 1:
            is_open = rows_of(source)
            tail = jnp.where(is_open, raw, tail)
            main = jnp.where(own_lanes(main_rows) | is_open, main, 0.0)
        return jnp.concatenate([main, tail], axis=0).astype(jnp.bfloat16)

    def gather(k, carry):
        g = partner(me // GROUP, k, groups)

        def wait_one(i, inner):
            source = g * GROUP + i

            @pl.when(source != me)
            def _():
                either(rows_of(source), lambda rows: copy_of(source, source, rows).wait_recv())

            return inner

        lax.fori_loop(0, GROUP, wait_one, 0)
        stacked = jnp.concatenate(
            [unpack(i, g * GROUP + i) for i in range(GROUP)], axis=1
        )
        moved = jnp.dot(stacked, place_ref[...], preferred_element_type=jnp.float32)
        start = g * (GROUP * pitch) + (lons - PATCH // 2)
        shift = lax.rem(start, 128)
        tile = lax.rem(start // 128, tiles)
        after = lax.rem(tile + 1, tiles)
        first_part = lane_of_pad >= shift
        for m in range(members):
            for q in range(PATCH):
                at = (m * PATCH + q) * 128
                value = pltpu.roll(moved[:, at : at + 128], shift, 1)
                rows = pl.ds(q, pad_rows, stride=PATCH)
                image_ref[m, tile, rows, :] += jnp.where(first_part, value, 0.0)
                image_ref[m, after, rows, :] += jnp.where(first_part, 0.0, value)
        return carry

    lane_of_pad = lax.broadcasted_iota(jnp.int32, (pad_rows, 128), 1)
    lax.fori_loop(0, groups, gather, 0)

    begin = 0 if own_rows % PATCH == 0 else lax.rem(me * own_rows, PATCH)
    for m in range(members):
        for tile in range(tiles):
            rows = image_ref[m, tile, pl.ds(begin, own_rows), :]
            out_ref[m, :, tile * 128 : (tile + 1) * 128] = rows.astype(jnp.bfloat16)

    def sent(r, carry):
        other = partner(me, r, windows)
        either(right_open, lambda rows: copy_of(me, other, rows).wait_send())
        return carry

    lax.fori_loop(1, windows, sent, 0)

    @pl.when(jnp.logical_not(right_open))
    def _():
        for index in range(up_tiles):
            edge_copy(index, edge_rows).wait_send()
        edge_copy(up_tiles, sf_tiles * part_rows).wait_send()


def tile_order(tiles):
    return (tiles - 2, 0, 2), (0, tiles - 2, 2)


def ranges_of(owners):
    ranges = []
    for o in owners:
        if ranges and ranges[-1][1] == o:
            ranges[-1][1] = o + 1
        else:
            ranges.append([o, o + 1])
    return ranges


def plan_of(spans, lat_rows, tiles):
    owners, depth = len(spans), LEVELS * lat_rows
    half, slots = owners // 2, -(-tiles // 2)
    sides = []
    for first, own in zip(tile_order(tiles), (range(half), range(half, owners))):
        done, sent, fresh = set(), set(), []
        for slot in range(slots):
            for t in range(first[slot], first[slot] + min(2, tiles - 2 * slot)):
                done.update(range(t * depth, (t + 1) * depth))
            if slot == slots - 1:
                done.update(range(tiles * depth, spans[-1][1]))
            new = [
                o for o in range(owners) if o not in sent and done.issuperset(range(*spans[o]))
            ]
            sent.update(new)
            fresh.append(([o for o in new if o in own], [o for o in new if o not in own]))
        sides.append(fresh)

    def both(slot, far, near):
        low, high = (ranges_of(side[slot][far]) for side in sides)
        count = max(len(low), len(high))
        low, high = (x + [[0, 0]] * (count - len(x)) for x in (low, high))
        return [(a, b, near) for a, b in zip(low, high)]

    sends = [both(0, 1, True)]
    for slot in range(1, slots):
        now = both(0, 0, None) if slot == 1 else []
        now += both(0, 1, False) if slot == 1 else []
        now += both(slot, 0, None)
        sends.append(now + both(slot, 1, None))
    return sends


def body(tokens, w_upper, w_surface, bias):
    members, tok_levels, lat_rows, lon_cols, width = tokens.shape
    windows = lax.axis_size("win")
    own_rows = CHANNELS * lat_rows * PATCH // windows
    lons = windows * lon_cols * PATCH
    spans = spans_of(windows, own_rows)
    longest = max(hi - lo for lo, hi in spans)
    main_rows = -(-3 * longest // 32) * 8
    extra_rows = max(longest - main_rows, 1)
    pad_rows = -(-longest // 16) * 16
    frame_rows = -(-(spans[-1][0] + pad_rows) // 8) * 8
    sends = plan_of(spans, lat_rows, w_upper.shape[1] // 128)
    edges = w_upper.shape[1] // 128 + 1
    bf16, f32 = jnp.bfloat16, jnp.float32
    by_lon = jnp.transpose(tokens, (0, 1, 3, 2, 4))
    return pl.pallas_call(
        functools.partial(kernel, (own_rows, main_rows, extra_rows, sends)),
        out_shape=pltpu.VMEM((members, own_rows, lons), bf16),
        in_specs=[pl.BlockSpec(memory_space=pltpu.HBM)] * 3
        + [pl.BlockSpec(memory_space=pltpu.SMEM)],
        out_specs=pl.BlockSpec(memory_space=pltpu.VMEM),
        scratch_shapes=[
            pltpu.VMEM(by_lon.shape, bf16),
            pltpu.VMEM(w_upper.shape, bf16),
            pltpu.VMEM(w_surface.shape, bf16),
            pltpu.VMEM((2, 2 * width, 256), bf16),
            pltpu.VMEM((members, 2, (tok_levels - 1) * lat_rows, 256), f32),
            pltpu.VMEM((frame_rows, 128), f32),
            pltpu.VMEM((windows, pad_rows, 128), bf16),
            pltpu.VMEM((windows, pad_rows, 128), bf16),
            pltpu.VMEM((edges, (tok_levels - 1) * lat_rows // 2, 128), bf16),
            pltpu.VMEM((edges, (tok_levels - 1) * lat_rows // 2, 128), bf16),
            pltpu.VMEM((128, 4 * 128), bf16),
            pltpu.VMEM((256, 1024), bf16),
            pltpu.VMEM((512, 256), bf16),
            pltpu.VMEM((GROUP * 128, members * PATCH * 128), bf16),
            pltpu.VMEM((members, lons // 128, pad_rows * PATCH, 128), f32),
            pltpu.VMEM((GROUP, pad_rows, 128), f32),
            pltpu.SemaphoreType.DMA((4,)),
            pltpu.SemaphoreType.DMA((windows,)),
            pltpu.SemaphoreType.DMA((windows,)),
            pltpu.SemaphoreType.DMA((2, edges)),
        ],
        compiler_params=pltpu.CompilerParams(
            collective_id=0, has_side_effects=True, vmem_limit_bytes=65 * 1000 * 1000
        ),
    )(by_lon, w_upper, w_surface, bias)


def solution(mesh):
    placed = (P("grp", None, None, "win", None), P(), P(), P())
    return jax.shard_map(
        body, mesh=mesh, in_specs=placed, out_specs=P("grp", "win", None), check_vma=False
    )
```

```python
import functools

import jax
import jax.numpy as jnp
from jax import lax
from jax.experimental import pallas as pl
from jax.experimental.pallas import tpu as pltpu
from jax.sharding import PartitionSpec as P

VARS_UP = 5
LEVELS = 13
VARS_SF = 4
PATCH = 4
GROUP = 8
TO_SPARE = (36, 32, 4)
CHANNELS = VARS_UP * LEVELS + VARS_SF


def spans_of(owners, own_rows):
    return [
        (o * own_rows // PATCH, -(-(o + 1) * own_rows // PATCH)) for o in range(owners)
    ]


def place_of(lane):
    return lane // 8 % 4, lane // 32 % 2 * 8 + lane % 8


def partner(me, r, windows):
    if windows & (windows - 1):
        return lax.rem(me + r, windows)
    return me ^ r


def kernel(
    plan, tok_hbm, wu_hbm, ws_hbm, bias_ref, out_ref,
    tok_ref, wu_ref, ws_ref, wb_ref, proj_ref, frame_ref, wire_ref, got_ref, edge_ref, side_ref, spot_ref,
    sel_ref, pick_ref,    place_ref, image_ref, wide_ref, load_sem, send_sem, recv_sem, edge_sem,
):
    members, tok_levels, lon_cols, lat_rows, width = tok_ref.shape
    windows, pad_rows, _ = wire_ref.shape
    half = windows // 2
    upper_levels = tok_levels - 1
    up_tiles = wu_ref.shape[1] // 128
    sf_tiles = ws_ref.shape[1] // 128
    me = lax.axis_index("win")
    own_rows, main_rows, extra_rows, sends = plan

    last = lon_cols - 1
    loads = [
        pltpu.make_async_copy(wu_hbm, wu_ref, load_sem.at[0]),
        pltpu.make_async_copy(ws_hbm, ws_ref, load_sem.at[1]),
        pltpu.make_async_copy(tok_hbm.at[:, :, last], tok_ref.at[:, :, last], load_sem.at[2]),
        pltpu.make_async_copy(
            tok_hbm.at[:, :, 0:last], tok_ref.at[:, :, 0:last], load_sem.at[3]
        ),
    ]
    for load in loads:
        load.start()

    barrier = pltpu.get_barrier_semaphore()

    def greet(r, carry):
        pl.semaphore_signal(
            barrier, inc=1, device_id={"win": partner(me, windows - r, windows)},
            device_id_type=pl.DeviceIdType.MESH,
        )
        return carry

    lax.fori_loop(1, windows, greet, 0)

    def iota(shape, axis):
        return lax.broadcasted_iota(jnp.int32, shape, axis)

    def one_hot(hit):
        return jnp.where(hit, 1.0, 0.0).astype(jnp.bfloat16)

    def second_of(lat, half):
        return (lat + 2 + 4 * half) % 8

    def source_of(tile, level, lat, lon):
        return tile * 128 + level * 64 + lat * 8 + lon

    for side in range(2):
        for near in range(2):
            row = iota((256, 256), 0)
            n = iota((256, 256), 1)
            k = side * 8 + n % 8 - PATCH * (side + near)
            lat = second_of(n // 8 % 4, n // 128)
            hit = row == source_of(n // 64 % 2, n // 32 % 2, lat, k)
            at = (2 * side + near) * 256
            sel_ref[:, at : at + 256] = one_hot(hit & (k >= 0) & (k < 2 * PATCH))
    row = iota(pick_ref.shape, 0)
    n = iota(pick_ref.shape, 1)
    lat = second_of(n // 4 % 4, n // 128)
    pick_ref[...] = one_hot(row == source_of(n // 32 % 4, n // 16 % 2, lat, n % 4 + PATCH))
    row = iota(spot_ref.shape, 0)
    n = iota(spot_ref.shape, 1)
    to_lane = row // 64 * 64 + row // 4 % 4 * 8 + row % 4
    spot_ref[...] = one_hot(n == row // 16 % 4 * 128 + to_lane)

    def spread(w):
        wide = jnp.dot(w, sel_ref[0 : w.shape[1], :], preferred_element_type=jnp.float32)
        for side in range(2):
            for near in range(2):
                at = (2 * side + near) * 256
                wb_ref[side, near * width : (near + 1) * width, :] = wide[
                    :, at : at + 256
                ].astype(jnp.bfloat16)

    lane = iota((lat_rows, 128), 1)
    line = iota((lat_rows, 128), 0)
    frame_lower = lane % 32 < 16
    edge_lower = lane % 16 < 8
    own_lane = place_of(lane)[1] < 12

    def own_lanes(rows):
        return place_of(iota((rows, 128), 1))[1] < 12

    def chunk_lanes(rows, c):
        return place_of(iota((rows, 128), 1))[1] // 4 == c

    def image(y, lower):
        first, second = y[:, :128], y[:, 128:]
        moved = jnp.where(
            lower, pltpu.roll(second, 1, 0), pltpu.roll(second, lat_rows - 1, 0)
        )
        keep = line != jnp.where(lower, 0, lat_rows - 1)
        return first + jnp.where(keep, moved, 0.0)

    def exchange(parts, wanted):
        at = iota(parts[0].shape, 1)
        low_half, even = at < 64, at // 32 % 2 == 0
        halves = []
        for h in range(-(-wanted // 2)):
            for a, b in ((parts[0], parts[2]), (parts[1], parts[3])):
                if h == 0:
                    halves.append(jnp.where(low_half, a, pltpu.roll(b, 64, 1)))
                else:
                    halves.append(jnp.where(low_half, pltpu.roll(a, 64, 1), b))
        out = []
        for p in range(wanted):
            a, b = halves[p // 2 * 2], halves[p // 2 * 2 + 1]
            if p % 2 == 0:
                out.append(jnp.where(even, a, pltpu.roll(b, 32, 1)))
            else:
                out.append(jnp.where(even, pltpu.roll(a, 96, 1), b))
        return out

    def put(channel, block):
        start = pl.multiple_of(channel * lat_rows, 8)
        frame_ref[pl.ds(start, lat_rows), :] = block + jnp.where(own_lane, bias_ref[channel], 0.0)

    def multiply(z0, z1):
        rows = (z1 - z0) * lat_rows
        for m in range(members):
            token = [tok_ref[m, z0:z1, j].reshape(rows, width) for j in range(lon_cols)]
            for side in range(2):
                proj_ref[m, side, 0:rows] = jnp.dot(
                    jnp.concatenate(token[side : side + 2], axis=1), wb_ref[side],
                    preferred_element_type=jnp.float32,
                )

    def merge(z, channels):
        at = slice(z * lat_rows, (z + 1) * lat_rows)
        parts = [
            image(proj_ref[m, side, at, :], frame_lower)
            for m in range(members)
            for side in range(2)
        ]
        for channel, block in zip(channels, exchange(parts, len(channels))):
            if channel is not None:
                put(channel, block)

    low = me < half

    def first_tile(slot):
        low_tiles, high_tiles = tile_order(up_tiles)
        return jnp.where(low, low_tiles[slot], high_tiles[slot])

    def tiles_of(slot):
        return min(2, up_tiles - 2 * slot)

    left_open = lax.rem(me, half) == 0
    right_open = lax.rem(me + 1, half) == 0

    def edge_copy(index, rows):
        return pltpu.make_async_remote_copy(
            src_ref=edge_ref.at[index, 0:rows],
            dst_ref=side_ref.at[index, 0:rows],
            send_sem=edge_sem.at[0, index],
            recv_sem=edge_sem.at[1, index],
            device_id={"win": lax.rem(me + 1, windows)},
            device_id_type=pl.DeviceIdType.MESH,
        )

    part_rows = lat_rows // 2
    edge_rows = upper_levels * part_rows

    def edges(w, z0, z1, put_edge):
        rows = (z1 - z0) * lat_rows
        weights = jnp.dot(w, pick_ref[0 : w.shape[1], :], preferred_element_type=jnp.float32)
        weights = weights.astype(jnp.bfloat16)
        for m in range(members):
            proj_ref[m, 0, 0:rows] = jnp.dot(
                tok_ref[m, z0:z1, last].reshape(rows, width), weights,
                preferred_element_type=jnp.float32,
            )
        for z in range(z1 - z0):
            parts = []
            for m in range(members):
                x = image(proj_ref[m, 0, z * lat_rows : (z + 1) * lat_rows, :], edge_lower)
                parts += [x[:part_rows], x[part_rows:]]
            for i, block in enumerate(exchange(parts, w.shape[1] // 128)):
                put_edge(i, z, block.astype(jnp.bfloat16))

    def make_edges():
        for load in loads[:3]:
            load.wait()
        for v in range(0, up_tiles, 4):

            def put_upper(i, z, block):
                edge_ref[v + i, z * part_rows : (z + 1) * part_rows] = block

            edges(wu_ref[:, v * 128 : min(v + 4, up_tiles) * 128], 0, upper_levels, put_upper)

        def put_surface(i, z, block):
            edge_ref[up_tiles, i * part_rows : (i + 1) * part_rows] = block

        edges(ws_ref[...], upper_levels, tok_levels, put_surface)

    def send_edges():
        @pl.when(jnp.logical_not(right_open))
        def _():
            for slot in range(slots):
                for i in range(tiles_of(slot)):
                    edge_copy(first_tile(slot) + i, edge_rows).start()
                if slot == slots - 1:
                    edge_copy(up_tiles, sf_tiles * part_rows).start()

    def take_edge(index, rows):
        edge_copy(index, rows).wait_recv()
        return jnp.dot(
            side_ref[index, 0:rows], spot_ref[...], preferred_element_type=jnp.float32
        )

    def add_rows(channel, h, block):
        at = pl.multiple_of(channel * lat_rows + h * part_rows, 8)
        frame_ref[pl.ds(at, part_rows), :] += block

    def take_upper(t):
        moved = take_edge(t, edge_rows)
        for z in range(upper_levels):
            for h in range(2):
                for l in range(min(2, LEVELS - 2 * z)):
                    lanes = (2 * h + l) * 128
                    block = moved[z * part_rows : (z + 1) * part_rows, lanes : lanes + 128]
                    add_rows(t * LEVELS + 2 * z + l, h, block)

    def take_surface():
        moved = take_edge(up_tiles, sf_tiles * part_rows)
        for i in range(sf_tiles):
            for h in range(2):
                for l in range(2):
                    lanes = (2 * h + l) * 128
                    block = moved[i * part_rows : (i + 1) * part_rows, lanes : lanes + 128]
                    add_rows(VARS_UP * LEVELS + 2 * i + l, h, block)

    def rows_of(window):
        return lax.rem(window + 1, half) == 0

    def copy_of(source, other, rows):
        return pltpu.make_async_remote_copy(
            src_ref=wire_ref.at[other, 0:rows],
            dst_ref=got_ref.at[source, 0:rows],
            send_sem=send_sem.at[other],
            recv_sem=recv_sem.at[source],
            device_id={"win": other},
            device_id_type=pl.DeviceIdType.MESH,
        )

    def either(is_open, run):
        @pl.when(is_open)
        def _():
            run(pad_rows)

        @pl.when(jnp.logical_not(is_open))
        def _():
            run(main_rows)

    def pack_into(ref, index, other):
        start = other * own_rows // PATCH
        main = frame_ref[pl.ds(start, main_rows), :]
        tail = frame_ref[pl.ds(start + main_rows, pad_rows - main_rows), :]
        chunks = []
        for c in range(3):
            first = c * extra_rows // 8 * 8
            end = min(-(-(c + 1) * extra_rows // 8) * 8, main_rows) if c < 2 else main_rows
            rows = frame_ref[pl.ds(start + main_rows - c * extra_rows + first, end - first), :]
            chunks.append((first, pltpu.roll(rows, TO_SPARE[c], 1)))
        line_of_8 = iota((8, 128), 0)
        spare = []
        for at in range(0, main_rows, 8):
            block = None
            for c, (first, rows) in enumerate(chunks):
                if first <= at < first + rows.shape[0]:
                    part = rows[at - first : at - first + 8]
                    begins = line_of_8 >= c * extra_rows - at
                    block = part if block is None else jnp.where(begins, part, block)
            spare.append(block)
        kept = own_lanes(main_rows) | right_open
        main = jnp.where(kept, main, jnp.concatenate(spare, axis=0))
        ref[index] = jnp.concatenate([main, tail], axis=0).astype(jnp.bfloat16)

    pair_of_me = me // 2

    def serve(low_range, high_range, near):
        begin, end = (jnp.where(low, a, b) for a, b in zip(low_range, high_range))
        first_pair = begin // 2
        pairs = (end + 1) // 2 - first_pair

        def send(i, carry):
            pair = first_pair + lax.rem(i + pair_of_me, jnp.maximum(pairs, 1))
            wanted = True if near is None else (lax.rem(pair // 2, 2) == lax.rem(pair_of_me // 2, 2)) == near

            @pl.when(wanted)
            def _():
                one, two = 2 * pair, 2 * pair + 1
                first, second = jnp.maximum(one, begin), jnp.minimum(two, end - 1)
                pack_into(wire_ref, first, first)
                pack_into(wire_ref, second, second)

                @pl.when((one != me) & (one >= begin))
                def _():
                    either(right_open, lambda rows: copy_of(me, one, rows).start())

                @pl.when((two != me) & (two < end))
                def _():
                    either(right_open, lambda rows: copy_of(me, two, rows).start())

            return carry

        lax.fori_loop(0, pairs, send, 0)

    slots = -(-up_tiles // 2)
    tiles = image_ref.shape[1]
    lons = tiles * 128
    groups = windows // GROUP
    pitch = lons // windows
    row = iota((128, place_ref.shape[1]), 0)
    col = iota(row.shape, 1)
    row_q, row_column = place_of(row)
    target = row // 64 * 512 + row_q * 128 + row_column

    def fill(i, carry):
        hit = (col == target + i * pitch) & ((row_column < 12) | (i == GROUP - 1))
        place_ref[pl.ds(pl.multiple_of(i * 128, 128), 128), :] = one_hot(hit)
        return carry

    lax.fori_loop(0, GROUP, fill, 0)
    image_ref[...] = jnp.zeros(image_ref.shape, jnp.float32)
    frame_ref[...] = jnp.zeros(frame_ref.shape, jnp.float32)
    def spread_upper(slot):
        t, count = first_tile(slot), tiles_of(slot)
        spread(wu_ref[:, pl.ds(pl.multiple_of(t * 128, 128), count * 128)])

    def meet():
        pl.semaphore_wait(barrier, windows - 1)
        send_edges()

    def settle(slot):
        @pl.when(jnp.logical_not(left_open))
        def _():
            for i in range(tiles_of(slot)):
                take_upper(first_tile(slot) + i)
            if slot == slots - 1:
                take_surface()

        for low_range, high_range, near in sends[slot]:
            serve(low_range, high_range, near)

    make_edges()
    spread_upper(0)
    early = me < windows // 4
    earliest = me < windows // 16
    pl.when(jnp.logical_not(early))(meet)
    loads[3].wait()
    for slot in range(slots):
        t, count = first_tile(slot), tiles_of(slot)
        if slot > 0:
            spread_upper(slot)
        multiply(0, upper_levels)
        for z in range(upper_levels):
            merge(
                z,
                [
                    (t + i) * LEVELS + 2 * z + l if 2 * z + l < LEVELS else None
                    for i in range(count)
                    for l in range(2)
                ],
            )
        if slot == slots - 1:
            spread(ws_ref[...])
            multiply(upper_levels, tok_levels)
            merge(0, [VARS_UP * LEVELS + v for v in range(VARS_SF)])

        if slot == 0:
            pl.when(early & jnp.logical_not(earliest))(meet)
            pl.when(jnp.logical_not(earliest))(functools.partial(settle, 0))
        else:
            if slot == 1:

                @pl.when(earliest)
                def _():
                    meet()
                    settle(0)

            settle(slot)
    pack_into(got_ref, me, me)

    def unpack(i, source):
        rows = got_ref[source].astype(jnp.float32)
        wide_ref[i] = rows
        main, raw = rows[:main_rows], rows[main_rows:]
        count = pad_rows - main_rows
        tail = jnp.zeros((count, 128), jnp.float32)
        for c in range(3):
            part = wide_ref[i, c * extra_rows : c * extra_rows + count]
            part = pltpu.roll(part, 128 - TO_SPARE[c], 1)
            tail = jnp.where(chunk_lanes(count, c), part, tail)
        if i == GROUP - 1:
            is_open = rows_of(source)
            tail = jnp.where(is_open, raw, tail)
            main = jnp.where(own_lanes(main_rows) | is_open, main, 0.0)
        return jnp.concatenate([main, tail], axis=0).astype(jnp.bfloat16)

    outer = (me < windows // 4) | (me >= windows - windows // 4)

    def gather(k, carry):
        g = partner(me // GROUP, jnp.where(outer & (k >= 2), groups + 1 - k, k), groups)

        def wait_one(i, inner):
            source = g * GROUP + i

            @pl.when(source != me)
            def _():
                either(rows_of(source), lambda rows: copy_of(source, source, rows).wait_recv())

            return inner

        lax.fori_loop(0, GROUP, wait_one, 0)
        stacked = jnp.concatenate(
            [unpack(i, g * GROUP + i) for i in range(GROUP)], axis=1
        )
        moved = jnp.dot(stacked, place_ref[...], preferred_element_type=jnp.float32)
        start = g * (GROUP * pitch) + (lons - PATCH // 2)
        shift = lax.rem(start, 128)
        tile = lax.rem(start // 128, tiles)
        after = lax.rem(tile + 1, tiles)
        first_part = lane_of_pad >= shift
        for m in range(members):
            for q in range(PATCH):
                at = (m * PATCH + q) * 128
                value = pltpu.roll(moved[:, at : at + 128], shift, 1)
                rows = pl.ds(q, pad_rows, stride=PATCH)
                image_ref[m, tile, rows, :] += jnp.where(first_part, value, 0.0)
                image_ref[m, after, rows, :] += jnp.where(first_part, 0.0, value)
        return carry

    lane_of_pad = lax.broadcasted_iota(jnp.int32, (pad_rows, 128), 1)
    lax.fori_loop(0, groups, gather, 0)

    begin = 0 if own_rows % PATCH == 0 else lax.rem(me * own_rows, PATCH)
    for m in range(members):
        for tile in range(tiles):
            rows = image_ref[m, tile, pl.ds(begin, own_rows), :]
            out_ref[m, :, tile * 128 : (tile + 1) * 128] = rows.astype(jnp.bfloat16)

    def sent(r, carry):
        other = partner(me, r, windows)
        either(right_open, lambda rows: copy_of(me, other, rows).wait_send())
        return carry

    lax.fori_loop(1, windows, sent, 0)

    @pl.when(jnp.logical_not(right_open))
    def _():
        for index in range(up_tiles):
            edge_copy(index, edge_rows).wait_send()
        edge_copy(up_tiles, sf_tiles * part_rows).wait_send()


def tile_order(tiles):
    return (tiles - 2, 0, 2), (0, tiles - 2, 2)


def ranges_of(owners):
    ranges = []
    for o in owners:
        if ranges and ranges[-1][1] == o:
            ranges[-1][1] = o + 1
        else:
            ranges.append([o, o + 1])
    return ranges


def plan_of(spans, lat_rows, tiles):
    owners, depth = len(spans), LEVELS * lat_rows
    half, slots = owners // 2, -(-tiles // 2)
    sides = []
    for first, own in zip(tile_order(tiles), (range(half), range(half, owners))):
        done, sent, fresh = set(), set(), []
        for slot in range(slots):
            for t in range(first[slot], first[slot] + min(2, tiles - 2 * slot)):
                done.update(range(t * depth, (t + 1) * depth))
            if slot == slots - 1:
                done.update(range(tiles * depth, spans[-1][1]))
            new = [
                o for o in range(owners) if o not in sent and done.issuperset(range(*spans[o]))
            ]
            sent.update(new)
            fresh.append(([o for o in new if o in own], [o for o in new if o not in own]))
        sides.append(fresh)

    def both(slot, far, near):
        low, high = (ranges_of(side[slot][far]) for side in sides)
        count = max(len(low), len(high))
        low, high = (x + [[0, 0]] * (count - len(x)) for x in (low, high))
        return [(a, b, near) for a, b in zip(low, high)]

    sends = [both(0, 1, True)]
    for slot in range(1, slots):
        now = both(0, 0, None) if slot == 1 else []
        now += both(0, 1, False) if slot == 1 else []
        now += both(slot, 0, None)
        sends.append(now + both(slot, 1, None))
    return sends


def body(tokens, w_upper, w_surface, bias):
    members, tok_levels, lat_rows, lon_cols, width = tokens.shape
    windows = lax.axis_size("win")
    own_rows = CHANNELS * lat_rows * PATCH // windows
    lons = windows * lon_cols * PATCH
    spans = spans_of(windows, own_rows)
    longest = max(hi - lo for lo, hi in spans)
    main_rows = -(-3 * longest // 32) * 8
    extra_rows = max(longest - main_rows, 1)
    pad_rows = -(-longest // 16) * 16
    frame_rows = -(-(spans[-1][0] + pad_rows) // 8) * 8
    sends = plan_of(spans, lat_rows, w_upper.shape[1] // 128)
    edges = w_upper.shape[1] // 128 + 1
    bf16, f32 = jnp.bfloat16, jnp.float32
    by_lon = jnp.transpose(tokens, (0, 1, 3, 2, 4))
    return pl.pallas_call(
        functools.partial(kernel, (own_rows, main_rows, extra_rows, sends)),
        out_shape=pltpu.VMEM((members, own_rows, lons), bf16),
        in_specs=[pl.BlockSpec(memory_space=pltpu.HBM)] * 3
        + [pl.BlockSpec(memory_space=pltpu.SMEM)],
        out_specs=pl.BlockSpec(memory_space=pltpu.VMEM),
        scratch_shapes=[
            pltpu.VMEM(by_lon.shape, bf16),
            pltpu.VMEM(w_upper.shape, bf16),
            pltpu.VMEM(w_surface.shape, bf16),
            pltpu.VMEM((2, 2 * width, 256), bf16),
            pltpu.VMEM((members, 2, (tok_levels - 1) * lat_rows, 256), f32),
            pltpu.VMEM((frame_rows, 128), f32),
            pltpu.VMEM((windows, pad_rows, 128), bf16),
            pltpu.VMEM((windows, pad_rows, 128), bf16),
            pltpu.VMEM((edges, (tok_levels - 1) * lat_rows // 2, 128), bf16),
            pltpu.VMEM((edges, (tok_levels - 1) * lat_rows // 2, 128), bf16),
            pltpu.VMEM((128, 4 * 128), bf16),
            pltpu.VMEM((256, 1024), bf16),
            pltpu.VMEM((512, 256), bf16),
            pltpu.VMEM((GROUP * 128, members * PATCH * 128), bf16),
            pltpu.VMEM((members, lons // 128, pad_rows * PATCH, 128), f32),
            pltpu.VMEM((GROUP, pad_rows, 128), f32),
            pltpu.SemaphoreType.DMA((4,)),
            pltpu.SemaphoreType.DMA((windows,)),
            pltpu.SemaphoreType.DMA((windows,)),
            pltpu.SemaphoreType.DMA((2, edges)),
        ],
        compiler_params=pltpu.CompilerParams(
            collective_id=0, has_side_effects=True, vmem_limit_bytes=65 * 1000 * 1000
        ),
    )(by_lon, w_upper, w_surface, bias)


def solution(mesh):
    placed = (P("grp", None, None, "win", None), P(), P(), P())
    return jax.shard_map(
        body, mesh=mesh, in_specs=placed, out_specs=P("grp", "win", None), check_vma=False
    )
```
